32 devices in a mesh: ens: 4 (over y, x), lon: 8 (over z, core).
Axes of the slice: x: 2, y: 2, z: 4, core: 2. Of those that a mesh axis runs over, the one named last changes fastest.
Arguments:
- control: float32 [8, 1024, 512], P('ens', None, 'lon'), may hold values from -6 to 6
- residual: float32 [8, 1024, 512], P('ens', None, 'lon'), may hold values from -6 to 6
- direction: float32 [8, 1024, 512], P('ens', None, 'lon'), may hold values from -6 to 6
- ens_perturb: bfloat16 [8, 3, 1024, 512], P('ens', None, None, 'lon'), may hold values from -1.5 to 1.5
- localize: float32 [1024, 1024], replicated, may hold values from -0.5 to 1.5
- obs_cell: int32 [32768], P('lon'), may hold values from 0 to 65535
- obs_slot: int32 [32768], P('lon'), may hold values from 0 to 3
- obs_weight: float32 [32768], P('lon'), may hold values from 0.5 to 4
Outputs:
- control_new: float32 [8, 1024, 512], P('ens', None, 'lon')
- residual_new: float32 [8, 1024, 512], P('ens', None, 'lon')
- direction_new: float32 [8, 1024, 512], P('ens', None, 'lon')
The draws below stay inside these ranges and needn't reach their ends.
Inputs may be any that keep to these rules, and one draw needn't show every extreme that they name: `obs_cell`: row-major cell within the entry's own longitude tile: row times 64 plus column. `obs_slot`: slot n < 3 observes the height after model step n + 1; slot 3 marks a padding entry that observes nothing.
All inputs are finite; a program needn't handle non-finite values.
Results may differ from the reference program's by a relative error of at most 0.0003.
Values sent between devices are 32-bit elements; how exact they have to be, the bound alone decides.
A program may use at most 64 MiB of HBM per device.

```python
import math
import jax
import jax.numpy as jnp
from jax import lax

LAT = 1024
CLON = 64
STEPS = 3
NOBS_DEV = 4096
MEMBERS = 8
LON = 512
NOBS = 32768


def draw_localize(key, part):
    row_ids = jnp.arange(LAT).astype(jnp.float32)
    distance = jnp.abs(row_ids[:, None] - row_ids[None, :])
    envelope = jnp.exp(-distance * 8.0 / LAT)
    jitter = 0.15 * jax.random.normal(key, (LAT, LAT), jnp.float32)
    jitter = jnp.clip(jitter, -0.5, 0.5)
    return jnp.eye(LAT, dtype=jnp.float32) + envelope * jitter


def place_ends(result, key, least, top_value):
    spot = [jax.random.randint(jax.random.fold_in(key, axis), (), 0, length) for axis, length in enumerate(result.shape)]
    main_axis = result.shape.index(max(result.shape))
    neighbour = spot[:main_axis] + [(spot[main_axis] + 1) % result.shape[main_axis]] + spot[main_axis + 1:]
    return result.at[tuple(spot)].set(least).at[tuple(neighbour)].set(top_value)


def levels(own_key, shape, split, least, largest):
    gain, own = 1.0, jax.random.fold_in(own_key, 6)
    for axis_at, blocks in split:
        draws = jnp.exp(jax.random.uniform(jax.random.fold_in(own, axis_at), (blocks,), jnp.float32, least / len(split), largest / len(split)))
        gain = gain * jnp.repeat(draws, shape[axis_at] // blocks).reshape([-1 if axis == axis_at else 1 for axis in range(len(shape))])
    return gain


def normal_values(own_key, dims, deviation, bound, split=(), held_as=jnp.bfloat16):
    gain = levels(own_key, dims, split, -0.22, 0.18) if split else 1.0
    result = jax.random.normal(own_key, dims, jnp.float32) * deviation * gain
    return jnp.minimum(jnp.maximum(result, -bound), bound).astype(held_as)


def setup_inputs(seed: int = 0) -> dict:
    keys = jax.random.split(jax.random.key(seed), 9)
    control = normal_values(keys[0], (MEMBERS, LAT, LON), 1.0, 6.0, ((0, 4), (2, 8)), jnp.float32)
    residual = normal_values(keys[1], (MEMBERS, LAT, LON), 1.0, 6.0, ((0, 4), (2, 8)), jnp.float32)
    direction = normal_values(keys[2], (MEMBERS, LAT, LON), 1.0, 6.0, ((0, 4), (2, 8)), jnp.float32)
    ens_perturb = normal_values(keys[3], (MEMBERS, 3, LAT, LON), 0.25, 1.5, ((0, 4), (3, 8)))
    localize = draw_localize(jax.random.fold_in(keys[8], 71), 0)
    obs_cell = place_ends(jax.random.randint(keys[5], (NOBS,), 0, LAT * CLON), jax.random.fold_in(keys[5], 1), 0, (LAT * CLON) - 1).astype(jnp.int32)
    obs_slot = place_ends(jax.random.randint(keys[6], (NOBS,), 0, STEPS + 1), jax.random.fold_in(keys[6], 1), 0, STEPS).astype(jnp.int32)
    obs_weight = jnp.clip(jnp.exp(math.log(4.0) - 2.0794415 * jax.random.uniform(keys[7], (NOBS,), jnp.float32) ** levels(keys[7], (NOBS,), ((0, 8),), -0.2, 0.2)), 0.5, 4.0)
    return {"control": control, "residual": residual, "direction": direction, "ens_perturb": ens_perturb, "localize": localize, "obs_cell": obs_cell, "obs_slot": obs_slot, "obs_weight": obs_weight}


wave_speed = 0.35
rotation = 0.2

def grid_factors(row_ids, lat_total):
    latitude = (-1.0 / 3.0 + 2.0 / 3.0 * (row_ids + 0.5) / lat_total) * jnp.pi
    return (1.0 / jnp.cos(latitude), jnp.sin(latitude))

def linear_step(fields, orient, metric, coriolis):
    height, zonal, meridional = (fields[0], fields[1], fields[2])

    def lon_diff(values):
        return 0.5 * metric[:, None] * (jnp.roll(values, -1, axis=1) - jnp.roll(values, 1, axis=1))

    def lat_diff(values):
        widened = jnp.pad(values, ((1, 1), (0, 0)))
        return 0.5 * (widened[2:] - widened[:-2])
    speed = orient * wave_speed
    turning = orient * rotation * coriolis[:, None]
    return jnp.stack([height - speed * (lon_diff(zonal) + lat_diff(meridional)), zonal - speed * lon_diff(height) + turning * meridional, meridional - speed * lat_diff(height) - turning * zonal])

def reference(control, residual, direction, ens_perturb, localize, obs_cell, obs_slot, obs_weight):
    hi = lax.Precision.HIGHEST
    row_ids = jnp.arange(LAT).astype(jnp.float32)
    metric, coriolis = grid_factors(row_ids, LAT)
    tile_index = (jnp.arange(obs_cell.shape[0]) // NOBS_DEV).astype(jnp.int32)
    cell_index = (obs_cell // CLON * LON + tile_index * CLON + obs_cell % CLON).astype(jnp.int32)

    def member_inc(accum, member_pair):
        member_pert, member_vec = member_pair
        localized = jnp.dot(localize, member_vec, precision=hi)
        return (accum + member_pert.astype(jnp.float32) * localized[None], None)
    increment, _ = lax.scan(member_inc, jnp.zeros((3, LAT, LON), jnp.float32), (ens_perturb, direction))
    tl_state = increment
    observed = jnp.zeros(obs_cell.shape, jnp.float32)
    for moment in range(STEPS):
        tl_state = linear_step(tl_state, 1.0, metric, coriolis)
        sampled = tl_state[0].reshape(-1)[cell_index]
        observed = jnp.where(obs_slot == moment, sampled, observed)
    weighted = obs_weight * observed
    adjoint = jnp.zeros((3, LAT, LON), jnp.float32)
    for moment in reversed(range(STEPS)):
        forcing = jnp.zeros((LAT * LON,), jnp.float32).at[cell_index].add(jnp.where(obs_slot == moment, weighted, 0.0))
        adjoint = adjoint.at[0].add(forcing.reshape(LAT, LON))
        adjoint = linear_step(adjoint, -1.0, metric, coriolis)

    def member_grad(carried, member_pert):
        projected = lax.optimization_barrier(jnp.sum(member_pert.astype(jnp.float32) * adjoint, axis=0))
        return (carried, jnp.dot(localize.T, projected, precision=hi))
    _, pulled_back = lax.scan(member_grad, jnp.float32(0.0), ens_perturb)
    image_vec = direction + pulled_back
    norm_old = jnp.sum(residual * residual)
    step_size = norm_old / jnp.sum(direction * image_vec)
    control_new = control + step_size * direction
    residual_new = residual - step_size * image_vec
    norm_new = jnp.sum(residual_new * residual_new)
    direction_new = residual_new + norm_new / norm_old * direction
    return (control_new, residual_new, direction_new)
```

```python
import functools
import itertools

import numpy as np
import jax
import jax.numpy as jnp
from jax import lax
from jax.experimental import pallas as pl
from jax.experimental.pallas import tpu as pltpu
from jax.sharding import PartitionSpec as P

STEPS = 3
HALO = 8
CHUNK = 1024
BLOCK = 256
MESH = pl.DeviceIdType.MESH
NT = (((1,), (1,)), ((), ()))
NN = (((1,), (0,)), ((), ()))


def split_bf16(values):
    high = values.astype(jnp.bfloat16)
    low = (values - high.astype(jnp.float32)).astype(jnp.bfloat16)
    return high, low


def dot(left, right, dims):
    return lax.dot_general(left, right, dims, preferred_element_type=jnp.float32)


def grid_constants(lat):
    phi = np.pi * (-1.0 / 3.0 + 2.0 / 3.0 * (np.arange(lat) + 0.5) / lat)
    half = 0.5 * 0.35
    up = np.full(lat, half)
    up[-1] = 0.0
    down = np.full(lat, half)
    down[0] = 0.0
    rows = np.stack([half / np.cos(phi), 0.2 * np.sin(phi), up, down])
    return np.ascontiguousarray(np.broadcast_to(rows[:, None], (4, 8, lat))).astype(np.float32)


def linear_step(source, target, sign, consts, blocks):
    rows, lat = source.shape[1], source.shape[2]
    lon_c, cor_c, up_c, down_c = (sign * consts[k] for k in range(4))
    for start in blocks:
        here = pl.ds(start, 8)

        def east(comp, block):
            if start + 8 == rows:
                return pltpu.roll(block, 7, 0)
            return source[comp, pl.ds(start + 1, 8), :]

        def west(comp, block):
            if start == 0:
                return pltpu.roll(block, 1, 0)
            return source[comp, pl.ds(start - 1, 8), :]

        def lat_diff(block):
            return up_c * pltpu.roll(block, lat - 1, 1) - down_c * pltpu.roll(block, 1, 1)

        height, zonal, merid = (source[c, here, :] for c in range(3))
        height_lon = east(0, height) - west(0, height)
        zonal_lon = east(1, zonal) - west(1, zonal)
        target[0, here, :] = height - lon_c * zonal_lon - lat_diff(merid)
        target[1, here, :] = zonal - lon_c * height_lon + cor_c * merid
        target[2, here, :] = merid - lat_diff(height) - cor_c * zonal


def grid_blocks(total, size):
    return range(0, total, size)


def row16(values):
    return jnp.broadcast_to(values, (16, values.shape[1])).astype(jnp.bfloat16)


def fold(values):
    values = values + pltpu.roll(values, 64, 1)
    return values + pltpu.roll(values, 32, 1)


def pack_rows(rows):
    lane = lax.broadcasted_iota(jnp.int32, (1, 128), 1) // 32
    packed = jnp.zeros((1, 128), jnp.float32)
    for k, row in enumerate(rows):
        packed = jnp.where(lane == k, fold(row), packed)
    return packed


def unpack_rows(total, number):
    lane = lax.broadcasted_iota(jnp.int32, (1, 128), 1) // 32
    return [
        jnp.sum(jnp.where(lane == k, total, 0.0), axis=1, keepdims=True) for k in range(number)
    ]


def lane_sum(values):
    total = values[:, :128]
    for k in range(128, values.shape[1], 128):
        total = total + values[:, k:k + 128]
    return total


def remote_count(ens, lat, nobs):
    return 2 * (lat // BLOCK) + (ens - 1) * (nobs // CHUNK) + 2 * STEPS


def kernel(
    ens, lon, direction_hbm, residual_hbm, perturb_hbm, localize_hbm, cell_hbm, slot_hbm,
    weight_hbm, consts_hbm,
    image, step_row, ratio_row,
    direction, localize, residual, perturb, cell, slot, weight, consts,
    high, low, split, onehot, fields, other, heights, observed, arrived, spread, forcing,
    tiles, tile, tiles2, tile2,
    load_sem, send_sem, recv_sem, tile_send, tile_recv, tile2_send, tile2_recv,
):
    me_e, me_l = lax.axis_index("ens"), lax.axis_index("lon")
    count = ens * lon
    me = me_e * lon + me_l
    members, cols, lat = direction.shape
    nobs = cell.shape[1]
    stacked = members * cols
    slots_cols = STEPS * cols
    blocks = [pl.ds(k, BLOCK) for k in grid_blocks(lat, BLOCK)]
    chunks = [pl.ds(k, CHUNK) for k in grid_blocks(nobs, CHUNK)]
    left_dev = (me_e, lax.rem(me_l + lon - 1, lon))
    right_dev = (me_e, lax.rem(me_l + 1, lon))

    load_ids = itertools.count()

    def load(src, dst):
        copy = pltpu.make_async_copy(src, dst, load_sem.at[next(load_ids)])
        copy.start()
        return copy

    load_obs = [load(cell_hbm, cell), load(slot_hbm, slot), load(weight_hbm, weight)]
    load_d = load(direction_hbm, direction)
    load_l = [load(localize_hbm.at[at, :], localize.at[at, :]) for at in blocks]
    load_p = load(perturb_hbm, perturb)
    load_c = load(consts_hbm, consts)
    load_r = load(residual_hbm, residual)

    barrier = pltpu.get_barrier_semaphore()

    def greet(offset, carry):
        peer = lax.rem(me + offset, count)
        pl.semaphore_signal(
            barrier, inc=1, device_id=(peer // lon, lax.rem(peer, lon)), device_id_type=MESH
        )
        return carry

    lax.fori_loop(1, count, greet, 0)

    ids = itertools.count()

    def remote(src, dst, device):
        k = next(ids)
        return pltpu.make_async_remote_copy(
            src_ref=src, dst_ref=dst, send_sem=send_sem.at[k], recv_sem=recv_sem.at[k],
            device_id=device, device_id_type=MESH,
        )

    def tell_all(source, target, send, recv):
        def tell(offset, carry):
            peer = lax.rem(me + offset, count)
            pltpu.make_async_remote_copy(
                src_ref=source, dst_ref=target.at[offset - 1], send_sem=send, recv_sem=recv,
                device_id=(peer // lon, lax.rem(peer, lon)), device_id_type=MESH,
            ).start()
            return carry

        lax.fori_loop(1, count, tell, 0)

    def hear_all(target, send, recv):
        everything = pltpu.make_async_remote_copy(
            src_ref=target, dst_ref=target, send_sem=send, recv_sem=recv,
            device_id=right_dev, device_id_type=MESH,
        )
        everything.wait_send()
        everything.wait_recv()

    for copy in load_obs:
        copy.wait()
    ids16 = lax.broadcasted_iota(jnp.int32, (16, 128), 0).astype(jnp.float32)
    tags = [(ids16 + 16.0 * g).astype(jnp.bfloat16) for g in range(BLOCK // 16)]
    one, zero = jnp.ones((16, 128), jnp.bfloat16), jnp.zeros((16, 128), jnp.bfloat16)

    def mark(step, carry):
        at = pl.ds(pl.multiple_of(step * 128, 128), 128)
        row = cell[:, at] // cols
        for b in grid_blocks(lat, BLOCK):
            inside = (row >= b) & (row < b + BLOCK)
            here = row16(jnp.where(inside, row - b, -1).astype(jnp.float32))
            for g in range(BLOCK // 16):
                onehot[pl.ds(b + 16 * g, 16), at] = jnp.where(here == tags[g], one, zero)
        return carry

    lax.fori_loop(0, nobs // 128, mark, 0)

    load_d.wait()
    d_high, d_low = split_bf16(direction[...].reshape(stacked, lat))
    split[pl.ds(0, stacked), :] = d_high
    split[pl.ds(stacked, stacked), :] = d_low

    edge = STEPS
    own = pl.ds(HALO, cols)
    first, last = pl.ds(HALO, edge), pl.ds(HALO + cols - edge, edge)
    before, after = pl.ds(HALO - edge, edge), pl.ds(HALO + cols, edge)

    def halo(ref, which, at):
        return (
            remote(ref.at[which, first, at], ref.at[which, after, at], left_dev),
            remote(ref.at[which, last, at], ref.at[which, before, at], right_dev),
        )

    f_copies = []
    for k, at in enumerate(blocks):
        load_l[k].wait()
        l_high, l_low = split_bf16(localize[at, :])
        high[at, :] = l_high
        low[at, :] = l_low
        both = dot(split[...], l_high, NT)
        local = both[:stacked] + both[stacked:] + dot(split[pl.ds(0, stacked), :], l_low, NT)
        if k == 0:
            load_p.wait()
        for c in range(3):
            total = None
            for m in range(members):
                term = perturb[m, c, :, at].astype(jnp.float32) * local[m * cols:(m + 1) * cols]
                total = term if total is None else total + term
            fields[c, own, at] = total
        if k == 0:
            pl.semaphore_wait(barrier, count - 1)
        for copy in halo(fields, pl.ds(0, 3), at):
            copy.start()
            f_copies.append(copy)

    load_c.wait()
    wide = fields.shape[1]

    def forward(source, target, n, blocks):
        linear_step(source, target, 1.0, consts, blocks)
        for start in blocks:
            if HALO <= start < HALO + cols:
                value = target[0, pl.ds(start, 8), :]
                v_high = value.astype(jnp.bfloat16).astype(jnp.float32)
                heights[pl.ds(n * cols + start - HALO, 8), :] = v_high
                heights[pl.ds(slots_cols + n * cols + start - HALO, 8), :] = value - v_high

    every = range(0, wide, 8)
    inside = [range(HALO + 8 * (n + 1), wide - HALO - 8 * (n + 1), 8) for n in range(STEPS)]
    outer = [[start for start in every if start not in inside[n]] for n in range(STEPS)]
    buffers = (fields, other, fields, other)
    for copy in f_copies:
        copy.wait_send()
    for n in range(STEPS):
        forward(buffers[n], buffers[n + 1], n, inside[n])

    load_r.wait()
    norms = [jnp.zeros((8, 128), jnp.float32)] * 2
    for at in blocks:
        for j, ref in enumerate((residual, direction)):
            value = ref[:, :, at]
            value = (value * value).reshape(stacked // 8, 8, BLOCK).sum(axis=0)
            norms[j] = norms[j] + lane_sum(value)
    norms = [jnp.sum(value, axis=0, keepdims=True) for value in norms]

    for copy in f_copies:
        copy.wait_recv()
    for n in range(STEPS):
        forward(buffers[n], buffers[n + 1], n, outer[n])

    def keys(at):
        cells, slots = cell[:, at], slot[:, at]
        return slots * cols + (cells - cells // cols * cols)

    peers = [(lax.rem(me_e + k, ens), me_l) for k in range(1, ens)]
    sums = {}
    table = heights[...].astype(jnp.bfloat16)
    key_ids = lax.broadcasted_iota(jnp.int32, (slots_cols, CHUNK), 0)
    for k, at in enumerate(chunks):
        both = dot(table, onehot[:, at], NN)
        both = both[:slots_cols] + both[slots_cols:]
        picked = jnp.where(key_ids == keys(at), both, 0.0)
        observed[:, at] = jnp.sum(picked, axis=0, keepdims=True)
        for j, peer in enumerate(peers):
            sums[j, k] = remote(observed.at[:, at], arrived.at[j, :, at], peer)
            sums[j, k].start()

    misfit = jnp.zeros((1, 128), jnp.float32)
    for k, at in enumerate(chunks):
        total = observed[:, at]
        for j in range(ens - 1):
            sums[j, k].wait_recv()
            total = total + arrived[j, :, at]
        weighted = weight[:, at] * total
        misfit = misfit + lane_sum(jnp.where(slot[:, at] < STEPS, weighted * total, 0.0))
        w_high = weighted.astype(jnp.bfloat16).astype(jnp.float32)
        w_low = weighted - w_high
        hit = key_ids == keys(at)
        left = jnp.concatenate(
            [jnp.where(hit, w_high, 0.0), jnp.where(hit, w_low, 0.0)], axis=0
        ).astype(jnp.bfloat16)
        both = dot(left, onehot[:, at], NT)
        both = both[:slots_cols] + both[slots_cols:]
        if k == 0:
            spread[...] = both
        else:
            spread[...] += both

    tile[...] = pack_rows([norms[0], norms[1], misfit * (1.0 / ens)])
    tell_all(tile, tiles, tile_send, tile_recv)

    for s in range(STEPS):
        forcing[s, own, :] = spread[pl.ds(s * cols, cols), :]
    w_copies = []
    for s in range(STEPS):
        for copy in halo(forcing, s, pl.ds(0, lat)):
            copy.start()
            w_copies.append(copy)

    for copy in w_copies:
        copy.wait()
    fields[0] = forcing[2]
    fields[1] = jnp.zeros_like(fields[1])
    fields[2] = jnp.zeros_like(fields[2])
    linear_step(fields, other, -1.0, consts, every)
    other[0] += forcing[1]
    linear_step(other, fields, -1.0, consts, every)
    fields[0] += forcing[0]
    linear_step(fields, other, -1.0, consts, every)

    for m in range(members):
        total = None
        for c in range(3):
            term = perturb[m, c].astype(jnp.float32) * other[c, own, :]
            total = term if total is None else total + term
        p_high, p_low = split_bf16(total)
        split[pl.ds(m * cols, cols), :] = p_high
        split[pl.ds(stacked + m * cols, cols), :] = p_low

    hear_all(tiles, tile_send, tile_recv)
    norm_old, square, misfit = unpack_rows(jnp.sum(tiles[...], axis=0) + tile[...], 3)
    step_size = norm_old / (square + misfit)

    def pulled(index, total):
        at = pl.ds(pl.multiple_of(index * BLOCK, BLOCK), BLOCK)
        both = dot(split[...], high[:, at], NN)
        back = both[:stacked] + both[stacked:] + dot(split[pl.ds(0, stacked), :], low[:, at], NN)
        d = direction[:, :, at].reshape(stacked, BLOCK)
        r = residual[:, :, at].reshape(stacked, BLOCK)
        img = d + back
        image[:, :, at] = img.reshape(members, cols, BLOCK)
        new = r - step_size * img
        return total + lane_sum((new * new).reshape(stacked // 8, 8, BLOCK).sum(axis=0))

    norm_new = lax.fori_loop(0, lat // BLOCK, pulled, jnp.zeros((8, 128), jnp.float32))
    tile2[...] = pack_rows([jnp.sum(norm_new, axis=0, keepdims=True)])
    tell_all(tile2, tiles2, tile2_send, tile2_recv)
    for copy in sums.values():
        copy.wait_send()
    hear_all(tiles2, tile2_send, tile2_recv)
    (norm_new,) = unpack_rows(jnp.sum(tiles2[...], axis=0) + tile2[...], 1)
    step_row[...] = jnp.broadcast_to(step_size, step_row.shape)
    ratio_row[...] = jnp.broadcast_to(norm_new / norm_old, ratio_row.shape)


def body(ens, lon, control, residual, direction, ens_perturb, localize, obs_cell, obs_slot, obs_weight):
    flip = functools.partial(jnp.swapaxes, axis1=-1, axis2=-2)
    control, residual, direction, ens_perturb = map(flip, (control, residual, direction, ens_perturb))
    members, cols, lat = direction.shape
    nobs = obs_cell.shape[0]
    count = ens * lon
    wide = cols + 2 * HALO
    f32, bf16, i32 = jnp.float32, jnp.bfloat16, jnp.int32
    vmem = pl.BlockSpec(memory_space=pltpu.VMEM)
    outside = pl.BlockSpec(memory_space=pl.ANY)
    dma = pltpu.SemaphoreType.DMA
    row = jax.ShapeDtypeStruct((1, lat), f32)
    copies = remote_count(ens, lat, nobs)
    image, step_size, ratio = pl.pallas_call(
        functools.partial(kernel, ens, lon),
        out_shape=(jax.ShapeDtypeStruct((members, cols, lat), f32), row, row),
        in_specs=[outside] * 8,
        out_specs=(vmem, vmem, vmem),
        scratch_shapes=[
            pltpu.VMEM((members, cols, lat), f32),
            pltpu.VMEM((lat, lat), f32),
            pltpu.VMEM((members, cols, lat), f32),
            pltpu.VMEM((members, 3, cols, lat), bf16),
            pltpu.VMEM((1, nobs), i32),
            pltpu.VMEM((1, nobs), i32),
            pltpu.VMEM((1, nobs), f32),
            pltpu.VMEM((4, 8, lat), f32),
            pltpu.VMEM((lat, lat), bf16),
            pltpu.VMEM((lat, lat), bf16),
            pltpu.VMEM((2 * members * cols, lat), bf16),
            pltpu.VMEM((lat, nobs), bf16),
            pltpu.VMEM((3, wide, lat), f32),
            pltpu.VMEM((3, wide, lat), f32),
            pltpu.VMEM((2 * STEPS * cols, lat), f32),
            pltpu.VMEM((1, nobs), f32),
            pltpu.VMEM((max(ens - 1, 1), 1, nobs), f32),
            pltpu.VMEM((STEPS * cols, lat), f32),
            pltpu.VMEM((STEPS, wide, lat), f32),
            pltpu.VMEM((count - 1, 1, 128), f32),
            pltpu.VMEM((1, 128), f32),
            pltpu.VMEM((count - 1, 1, 128), f32),
            pltpu.VMEM((1, 128), f32),
            dma((7 + lat // BLOCK,)), dma((copies,)), dma((copies,)),
            dma, dma, dma, dma,
        ],
        compiler_params=pltpu.CompilerParams(collective_id=0, has_side_effects=True),
    )(
        direction, residual, ens_perturb, localize,
        obs_cell.reshape(1, nobs), obs_slot.reshape(1, nobs), obs_weight.reshape(1, nobs),
        jnp.asarray(grid_constants(lat)),
    )
    control_new = control + step_size * direction
    residual_new = residual - step_size * image
    direction_new = residual_new + ratio * direction
    return tuple(map(flip, (control_new, residual_new, direction_new)))


def solution(mesh):
    fields = P("ens", None, "lon")
    in_specs = (fields, fields, fields, P("ens", None, None, "lon"), P(), P("lon"), P("lon"), P("lon"))
    ens, lon = mesh.shape["ens"], mesh.shape["lon"]
    return jax.shard_map(
        functools.partial(body, ens, lon), mesh=mesh, in_specs=in_specs,
        out_specs=(fields, fields, fields), check_vma=False,
    )
```

```python
import functools
import itertools

import numpy as np
import jax
import jax.numpy as jnp
from jax import lax
from jax.experimental import pallas as pl
from jax.experimental.pallas import tpu as pltpu
from jax.sharding import PartitionSpec as P

STEPS = 3
HALO = 8
CHUNK = 2048
BLOCK = 256
MESH = pl.DeviceIdType.MESH
NT = (((1,), (1,)), ((), ()))
NN = (((1,), (0,)), ((), ()))


def split_bf16(values):
    high = values.astype(jnp.bfloat16)
    low = (values - high.astype(jnp.float32)).astype(jnp.bfloat16)
    return high, low


def dot(left, right, dims):
    return lax.dot_general(left, right, dims, preferred_element_type=jnp.float32)


def grid_constants(lat):
    phi = np.pi * (-1.0 / 3.0 + 2.0 / 3.0 * (np.arange(lat) + 0.5) / lat)
    half = 0.5 * 0.35
    up = np.full(lat, half)
    up[-1] = 0.0
    down = np.full(lat, half)
    down[0] = 0.0
    rows = np.stack([half / np.cos(phi), 0.2 * np.sin(phi), up, down])
    return np.ascontiguousarray(np.broadcast_to(rows[:, None], (4, 8, lat))).astype(np.float32)


def linear_step(source, target, sign, consts, blocks, low_end, high_end, rest=True, extra=None):
    lat = source.shape[2]
    lon_c, cor_c, up_c, down_c = (consts[k] for k in range(4))

    def less(value, term):
        return value - term if sign > 0 else value + term

    for start in blocks:
        here = pl.ds(start, 8)

        def lon_diff(comp, block):
            if start + 8 == high_end:
                east = pltpu.roll(block, 7, 0)
            else:
                east = source[comp, pl.ds(start + 1, 8), :]
            if start == low_end:
                west = pltpu.roll(block, 1, 0)
            else:
                west = source[comp, pl.ds(start - 1, 8), :]
            return lon_c * (east - west)

        def lat_diff(block):
            return up_c * pltpu.roll(block, lat - 1, 1) - down_c * pltpu.roll(block, 1, 1)

        height = source[0, here, :]
        along_lon, along_lat = lon_diff(0, height), lat_diff(height)
        if rest:
            zonal, merid = source[1, here, :], source[2, here, :]
            new = less(height, lon_diff(1, zonal) + lat_diff(merid))
            target[1, here, :] = less(zonal, along_lon - cor_c * merid)
            target[2, here, :] = less(merid, along_lat + cor_c * zonal)
        else:
            new = height
            target[1, here, :] = less(0.0, along_lon)
            target[2, here, :] = less(0.0, along_lat)
        target[0, here, :] = new if extra is None else new + extra[here, :]


def fold(values):
    values = values + pltpu.roll(values, 64, 1)
    return values + pltpu.roll(values, 32, 1)


def pack_rows(rows):
    lane = lax.broadcasted_iota(jnp.int32, (1, 128), 1) // 32
    packed = jnp.zeros((1, 128), jnp.float32)
    for k, row in enumerate(rows):
        packed = jnp.where(lane == k, fold(row), packed)
    return packed


def unpack_rows(total, number):
    lane = lax.broadcasted_iota(jnp.int32, (1, 128), 1) // 32
    return [
        jnp.sum(jnp.where(lane == k, total, 0.0), axis=1, keepdims=True) for k in range(number)
    ]


def lane_sum(values):
    total = values[:, :128]
    for k in range(128, values.shape[1], 128):
        total = total + values[:, k:k + 128]
    return total


def remote_count(ens, lat, nobs):
    return 4 + (ens - 1) * (1 + nobs // CHUNK)


def side_rows():
    return [(n, k) for n in reversed(range(STEPS)) for k in range(n + 1)]


def kernel(
    ens, lon, control_hbm, direction_hbm, residual_hbm, perturb_hbm, localize_hbm, cell_hbm,
    slot_hbm, weight_hbm, consts_hbm,
    control, residual, direction, image, scalars,
    localize, perturb, cell, slot, weight, consts,
    high, low, split, onehot, state0, state1, state2, state3, heights, observed, arrived,
    spread, forcing, near, near_in, mass, mass_in, tiles, tile,
    load_sem, send_sem, recv_sem, tile_send, tile_recv,
):
    me_e, me_l = lax.axis_index("ens"), lax.axis_index("lon")
    members, cols, lat = direction.shape
    nobs = cell.shape[1]
    wide = state0.shape[1]
    stacked = members * cols
    slots_cols = STEPS * cols
    blocks = [pl.ds(k, BLOCK) for k in range(0, lat, BLOCK)]
    chunks = [pl.ds(k, CHUNK) for k in range(0, nobs, CHUNK)]
    panels = range(lat // 128)

    def wrap(value, size):
        return jnp.where(value >= size, value - size, value)

    left_dev = (me_e, wrap(me_l + lon - 1, lon))
    right_dev = (me_e, wrap(me_l + 1, lon))

    load_ids = itertools.count()

    def load(src, dst):
        copy = pltpu.make_async_copy(src, dst, load_sem.at[next(load_ids)])
        copy.start()
        return copy

    load_obs = [load(cell_hbm, cell), load(slot_hbm, slot), load(weight_hbm, weight)]
    load_d = load(direction_hbm, direction)
    load_l = [load(localize_hbm.at[at, :], localize.at[at, :]) for at in blocks]
    load_p = load(perturb_hbm, perturb)
    load_c = load(consts_hbm, consts)
    load_r = load(residual_hbm, residual)
    load_v = load(control_hbm, control)

    barrier = pltpu.get_barrier_semaphore()
    ids = itertools.count()

    def remote(src, dst, device):
        k = next(ids)
        return pltpu.make_async_remote_copy(
            src_ref=src, dst_ref=dst, send_sem=send_sem.at[k], recv_sem=recv_sem.at[k],
            device_id=device, device_id_type=MESH,
        )

    def each_peer(act):
        for e in range(ens):
            peer_e = wrap(me_e + e, ens)

            def visit(l, carry):
                act(e * lon + l - 1, (peer_e, wrap(me_l + l, lon)))
                return carry

            lax.fori_loop(0 if e else 1, lon, visit, 0, unroll=True)

    each_peer(lambda index, device: pl.semaphore_signal(
        barrier, inc=1, device_id=device, device_id_type=MESH
    ))

    for copy in load_obs:
        copy.wait()
    rows = (cell[...] // cols).reshape(nobs // 128, 128)
    rows = jnp.concatenate([rows] * (128 * 128 // nobs), axis=0).T
    lanes = lax.broadcasted_iota(jnp.int32, (16, 128), 1).astype(jnp.int16)
    one, zero = jnp.ones((16, 128), jnp.bfloat16), jnp.zeros((16, 128), jnp.bfloat16)
    for group in range(nobs // 128):
        for s in range(0, 128, 16):
            row = jnp.broadcast_to(rows[s:s + 16, group:group + 1], (16, 128)).astype(jnp.int16)
            for j in panels:
                hit = row == lanes + jnp.int16(128 * j)
                onehot[j, pl.ds(128 * group + s, 16), :] = jnp.where(hit, one, zero)

    def panel(ref, at, which=panels):
        return jnp.concatenate([ref[j, at, :] for j in which], axis=1)

    def store_panels(ref, at, values):
        for j in panels:
            ref[j, at, :] = values[:, 128 * j:128 * j + 128]

    load_d.wait()
    d_high, d_low = split_bf16(direction[...].reshape(stacked, lat))

    edge = 2 * STEPS
    own = pl.ds(HALO, cols)
    first, last = pl.ds(HALO, edge), pl.ds(HALO + cols - edge, edge)
    before, after = pl.ds(HALO - edge, edge), pl.ds(HALO + cols, edge)
    d_both = jnp.concatenate([d_high, d_low], axis=0)
    for copy in load_l:
        copy.wait()
    load_p.wait()
    for at in blocks:
        l_high, l_low = split_bf16(localize[at, :])
        store_panels(high, at, l_high)
        store_panels(low, at, l_low)
        both = dot(d_both, l_high, NT)
        local = both[:stacked] + both[stacked:] + dot(d_high, l_low, NT)
        for c in range(3):
            total = None
            for m in range(members):
                term = perturb[m, c, :, at].astype(jnp.float32) * local[m * cols:(m + 1) * cols]
                total = term if total is None else total + term
            state0[c, own, at] = total
    pl.semaphore_wait(barrier, ens * lon - 1)
    f_copies = [
        remote(state0.at[:, first], state0.at[:, after], left_dev),
        remote(state0.at[:, last], state0.at[:, before], right_dev),
    ]
    for copy in f_copies:
        copy.start()

    load_c.wait()
    states = (state0, state1, state2, state3)
    edge_rows = 2 * 8 * STEPS
    mid_rows = slots_cols - edge_rows

    def keep(n, starts):
        for start in starts:
            value = states[n + 1][0, pl.ds(start, 8), :]
            v_high = value.astype(jnp.bfloat16).astype(jnp.float32)
            if start == HALO or start == HALO + cols - 8:
                row, step = n * 16 + (8 if start > HALO else 0), edge_rows
            else:
                row, step = 2 * edge_rows + n * (cols - 16) + start - HALO - 8, mid_rows
            heights[pl.ds(row, 8), :] = v_high
            heights[pl.ds(row + step, 8), :] = value - v_high

    mid = range(HALO + 8, HALO + cols - 8, 8)
    for n in range(STEPS):
        starts = range(HALO, HALO + cols, 8) if n < STEPS - 1 else mid
        linear_step(states[n], states[n + 1], 1, consts, starts, HALO, HALO + cols)
        keep(n, mid)

    def keys(at):
        cells, slots = cell[:, at], slot[:, at]
        return slots * cols + (cells - cells // cols * cols)

    def scattered(hit, values):
        v_high = values.astype(jnp.bfloat16).astype(jnp.float32)
        return jnp.concatenate(
            [jnp.where(hit, v_high, 0.0), jnp.where(hit, values - v_high, 0.0)], axis=0
        ).astype(jnp.bfloat16)

    def picked(rows_at, at, count, ids_of):
        table = heights[rows_at, :].astype(jnp.bfloat16)
        both = dot(table, panel(onehot, at), NT)
        both = both[:count] + both[count:]
        ids = lax.broadcasted_iota(jnp.int32, both.shape, 0)
        cells, slots = cell[:, at], slot[:, at]
        key = ids_of(slots, cells - cells // cols * cols)
        return jnp.sum(jnp.where(ids == key, both, 0.0), axis=0, keepdims=True)

    def mid_ids(slots, col):
        inside = (col >= 8) & (col < cols - 8)
        return jnp.where(inside, slots * (cols - 16) + col - 8, -1)

    def edge_ids(slots, col):
        place = jnp.where(col < 8, col, col - (cols - 16))
        return jnp.where((col >= 8) & (col < cols - 8), -1, slots * 16 + place)

    def kept(ids_of, count):
        def ids(slots, col):
            key = ids_of(slots, col)
            return jnp.where(slots < STEPS, key, -1)
        return ids

    for at in chunks:
        observed[:, at] = picked(
            pl.ds(2 * edge_rows, 2 * mid_rows), at, mid_rows, kept(mid_ids, mid_rows)
        )

    load_r.wait()
    norm_old = jnp.zeros((8, 128), jnp.float32)
    for at in blocks:
        value = residual[:, :, at]
        norm_old += lane_sum((value * value).reshape(stacked // 8, 8, BLOCK).sum(axis=0))

    for copy in f_copies:
        copy.wait_recv()
    ends = (0, HALO, HALO + cols - 8, HALO + cols)
    for n in range(STEPS):
        linear_step(states[n], states[n + 1], 1, consts, ends, 0, wide)
        keep(n, (HALO, HALO + cols - 8))
    used = pl.ds(0, len(side_rows()))
    peers = [(wrap(me_e + k, ens), me_l) for k in range(1, ens)]
    for k, (n, dist) in enumerate(side_rows()):
        near[0, pl.ds(k, 1), :] = states[n + 1][0, pl.ds(HALO - 1 - n + dist, 1), :]
        near[1, pl.ds(k, 1), :] = states[n + 1][0, pl.ds(HALO + cols + dist, 1), :]
    n_copies = [
        remote(near.at[:, used], near_in.at[j, :, used], peer) for j, peer in enumerate(peers)
    ]

    sums = {}
    for k, at in enumerate(chunks):
        observed[:, at] += picked(pl.ds(0, 2 * edge_rows), at, edge_rows, kept(edge_ids, edge_rows))
        for j, peer in enumerate(peers):
            sums[j, k] = remote(observed.at[:, at], arrived.at[j, :, at], peer)
            sums[j, k].start()
    for copy in n_copies:
        copy.start()

    def side_ids(width):
        row = lax.broadcasted_iota(jnp.int32, (16, 128), 0)
        result = jnp.full((16, 128), -1, jnp.int32)
        for k, (n, dist) in enumerate(side_rows()):
            result = jnp.where(row == k, n * cols + dist, result)
            result = jnp.where(row == 8 + k, n * cols + cols - 1 - n + dist, result)
        return jnp.concatenate([result] * (width // 128), axis=1)

    left = scattered(side_ids(nobs) == keys(pl.ds(0, nobs)), weight[...])
    both = dot(left, panel(onehot, pl.ds(0, nobs)), NN)
    mass[...] = (both[:16] + both[16:]).reshape(2, 8, lat)
    m_copies = [
        remote(mass.at[0, used], mass_in.at[1, used], left_dev),
        remote(mass.at[1, used], mass_in.at[0, used], right_dev),
    ]
    for copy in m_copies:
        copy.start()

    key_ids = lax.broadcasted_iota(jnp.int32, (slots_cols, CHUNK), 0)
    for k, at in enumerate(chunks):
        total = observed[:, at]
        for j in range(ens - 1):
            sums[j, k].wait_recv()
            total = total + arrived[j, :, at]
        left = scattered(key_ids == keys(at), weight[:, at] * total)
        both = dot(left, panel(onehot, at), NN)
        both = both[:slots_cols] + both[slots_cols:]
        if k == 0:
            spread[...] = both
        elif k < len(chunks) - 1:
            spread[...] += both
        else:
            both = spread[...] + both
            for s in range(STEPS):
                forcing[s, own, :] = both[s * cols:(s + 1) * cols]

    for copy in m_copies + n_copies:
        copy.wait_recv()
    for side in range(2):
        total = near[side]
        for j in range(ens - 1):
            total = total + near_in[j, side]
        total = total * mass_in[side]
        for k, (n, dist) in enumerate(side_rows()):
            row = HALO + cols + dist if side else HALO - 1 - n + dist
            forcing[n, pl.ds(row, 1), :] = total[k:k + 1]
    every = range(0, wide, 8)
    inner = range(HALO, HALO + cols, 8)
    linear_step(forcing.at[pl.ds(2, 1)], state1, -1, consts, every, 0, wide, False, forcing.at[1])
    linear_step(state1, state2, -1, consts, every, 0, wide, True, forcing.at[0])
    linear_step(state2, state3, -1, consts, inner, 0, wide)

    for m in range(members):
        total = None
        for c in range(3):
            term = perturb[m, c].astype(jnp.float32) * state3[c, own, :]
            total = term if total is None else total + term
        p_high, p_low = split_bf16(total)
        store_panels(split, pl.ds(m * cols, cols), p_high)
        store_panels(split, pl.ds(stacked + m * cols, cols), p_low)

    p_both = panel(split, pl.ds(0, 2 * stacked))
    sums_new = [norm_old] + [jnp.zeros((8, 128), jnp.float32)] * 3
    for k, at in enumerate(blocks):
        pair = range(k * BLOCK // 128, (k + 1) * BLOCK // 128)
        both = dot(p_both, panel(high, pl.ds(0, lat), pair), NN)
        back = both[:stacked] + both[stacked:]
        back += dot(p_both[:stacked], panel(low, pl.ds(0, lat), pair), NN)
        d = direction[:, :, at].reshape(stacked, BLOCK)
        r = residual[:, :, at].reshape(stacked, BLOCK)
        img = d + back
        image[:, :, at] = img.reshape(members, cols, BLOCK)
        for j, term in enumerate((d * img, r * img, img * img)):
            sums_new[j + 1] += lane_sum(term.reshape(stacked // 8, 8, BLOCK).sum(axis=0))

    tile[...] = pack_rows([jnp.sum(value, axis=0, keepdims=True) for value in sums_new])

    def tell(index, device):
        pltpu.make_async_remote_copy(
            src_ref=tile, dst_ref=tiles.at[index], send_sem=tile_send, recv_sem=tile_recv,
            device_id=device, device_id_type=MESH,
        ).start()

    each_peer(tell)
    load_v.wait()
    for copy in f_copies + m_copies + n_copies + list(sums.values()):
        copy.wait_send()
    everything = pltpu.make_async_remote_copy(
        src_ref=tiles, dst_ref=tiles, send_sem=tile_send, recv_sem=tile_recv,
        device_id=right_dev, device_id_type=MESH,
    )
    everything.wait_send()
    everything.wait_recv()
    norm_old, curvature, cross_term, square = unpack_rows(
        jnp.sum(tiles[...], axis=0) + tile[...], 4
    )
    step_size = norm_old / curvature
    norm_new = norm_old - 2.0 * step_size * cross_term + step_size * step_size * square
    scalars[pl.ds(0, 1), :] = jnp.broadcast_to(step_size, (1, 128))
    scalars[pl.ds(1, 1), :] = jnp.broadcast_to(norm_new / norm_old, (1, 128))


def update(
    control, residual, direction, image, scalars, control_out, residual_out, direction_out,
    control_new, residual_new, direction_new, sem,
):
    step_size, ratio = scalars[pl.ds(0, 1), pl.ds(0, 1)], scalars[pl.ds(1, 1), pl.ds(0, 1)]
    ids = itertools.count()
    copies = []

    def send(src, dst, at):
        copies.append(pltpu.make_async_copy(src.at[at], dst.at[at], sem.at[next(ids)]))
        copies[-1].start()

    members, cols = control.shape[:2]
    for m in range(members):
        for h in range(2):
            at = (m, pl.ds(h * cols // 2, cols // 2))
            d = direction[at]
            new = residual[at] - step_size * image[at]
            residual_new[at] = new
            direction_new[at] = new + ratio * d
            control_new[at] = control[at] + step_size * d
            send(residual_new, residual_out, at)
            send(direction_new, direction_out, at)
            send(control_new, control_out, at)
    for copy in copies:
        copy.wait()


def body(ens, lon, control, residual, direction, ens_perturb, localize, obs_cell, obs_slot, obs_weight):
    flip = functools.partial(jnp.swapaxes, axis1=-1, axis2=-2)
    control, residual, direction, ens_perturb = map(flip, (control, residual, direction, ens_perturb))
    members, cols, lat = direction.shape
    nobs = obs_cell.shape[0]
    count = ens * lon
    wide = cols + 2 * HALO
    f32, bf16, i32 = jnp.float32, jnp.bfloat16, jnp.int32
    hbm = pl.BlockSpec(memory_space=pltpu.HBM)
    dma = pltpu.SemaphoreType.DMA
    field = pltpu.VMEM((members, cols, lat), f32)
    vmem = pl.BlockSpec(memory_space=pltpu.VMEM)
    copies = remote_count(ens, lat, nobs)
    outs = pl.pallas_call(
        functools.partial(kernel, ens, lon),
        out_shape=(field, field, field, field, pltpu.VMEM((8, 128), f32)),
        in_specs=[hbm] * 9,
        out_specs=(vmem,) * 5,
        scratch_shapes=[
            pltpu.VMEM((lat, lat), f32),
            pltpu.VMEM((members, 3, cols, lat), bf16),
            pltpu.VMEM((1, nobs), i32),
            pltpu.VMEM((1, nobs), i32),
            pltpu.VMEM((1, nobs), f32),
            pltpu.VMEM((4, 8, lat), f32),
            pltpu.VMEM((lat // 128, lat, 128), bf16),
            pltpu.VMEM((lat // 128, lat, 128), bf16),
            pltpu.VMEM((lat // 128, 2 * members * cols, 128), bf16),
            pltpu.VMEM((lat // 128, nobs, 128), bf16),
            pltpu.VMEM((3, wide, lat), f32),
            pltpu.VMEM((3, wide, lat), f32),
            pltpu.VMEM((3, wide, lat), f32),
            pltpu.VMEM((3, wide, lat), f32),
            pltpu.VMEM((2 * STEPS * cols, lat), f32),
            pltpu.VMEM((1, nobs), f32),
            pltpu.VMEM((max(ens - 1, 1), 1, nobs), f32),
            pltpu.VMEM((STEPS * cols, lat), f32),
            pltpu.VMEM((STEPS, wide, lat), f32),
            pltpu.VMEM((2, 8, lat), f32),
            pltpu.VMEM((max(ens - 1, 1), 2, 8, lat), f32),
            pltpu.VMEM((2, 8, lat), f32),
            pltpu.VMEM((2, 8, lat), f32),
            pltpu.VMEM((count - 1, 1, 128), f32),
            pltpu.VMEM((1, 128), f32),
            dma((8 + lat // BLOCK,)), dma((copies,)), dma((copies,)),
            dma, dma,
        ],
        compiler_params=pltpu.CompilerParams(
            collective_id=0, has_side_effects=True, vmem_limit_bytes=61 * 1024 * 1024
        ),
    )(
        control, direction, residual, ens_perturb, localize,
        obs_cell.reshape(1, nobs), obs_slot.reshape(1, nobs), obs_weight.reshape(1, nobs),
        jnp.asarray(grid_constants(lat)),
    )
    outs = pl.pallas_call(
        update,
        out_shape=[jax.ShapeDtypeStruct((members, cols, lat), f32)] * 3,
        in_specs=[vmem] * 5,
        out_specs=[hbm] * 3,
        scratch_shapes=[pltpu.VMEM((members, cols, lat), f32)] * 3 + [dma((6 * members,))],
        compiler_params=pltpu.CompilerParams(vmem_limit_bytes=8 * 1024 * 1024),
    )(*outs)
    return tuple(map(flip, outs))


def solution(mesh):
    fields = P("ens", None, "lon")
    in_specs = (fields, fields, fields, P("ens", None, None, "lon"), P(), P("lon"), P("lon"), P("lon"))
    ens, lon = mesh.shape["ens"], mesh.shape["lon"]
    return jax.shard_map(
        functools.partial(body, ens, lon), mesh=mesh, in_specs=in_specs,
        out_specs=(fields, fields, fields), check_vma=False,
    )
```

```python
import functools
import itertools

import numpy as np
import jax
import jax.numpy as jnp
from jax import lax
from jax.experimental import pallas as pl
from jax.experimental.pallas import tpu as pltpu
from jax.sharding import PartitionSpec as P

STEPS = 3
HALO = 8
HALF = 0.5 * 0.35
SHARES = (0, 2, 4, 6, 8)
BLOCK = 256
MESH = pl.DeviceIdType.MESH
NT = (((1,), (1,)), ((), ()))
NN = (((1,), (0,)), ((), ()))


def split_bf16(values):
    high = values.astype(jnp.bfloat16)
    low = (values - high.astype(jnp.float32)).astype(jnp.bfloat16)
    return high, low


def dot(left, right, dims):
    return lax.dot_general(left, right, dims, preferred_element_type=jnp.float32)


def grid_constants(lat):
    phi = np.pi * (-1.0 / 3.0 + 2.0 / 3.0 * (np.arange(lat) + 0.5) / lat)
    rows = np.stack([HALF / np.cos(phi), 0.2 * np.sin(phi)])
    return np.ascontiguousarray(np.broadcast_to(rows[:, None], (2, 8, lat))).astype(np.float32)


def linear_step(source, target, sign, consts, blocks, low_end, high_end, rest=True, extra=None):
    lat = source.shape[2]
    lon_c, cor_c = consts[0], consts[1]
    lane = lax.broadcasted_iota(jnp.int32, (8, 128), 1)

    def less(value, term):
        return value - term if sign > 0 else value + term

    for start in blocks:
        here = pl.ds(start, 8)

        def lon_diff(comp, block):
            if start + 8 == high_end:
                east = pltpu.roll(block, 7, 0)
            else:
                east = source[comp, pl.ds(start + 1, 8), :]
            if start == low_end:
                west = pltpu.roll(block, 1, 0)
            else:
                west = source[comp, pl.ds(start - 1, 8), :]
            return lon_c * (east - west)

        def lat_diff(block):
            up, down = pltpu.roll(block, lat - 1, 1), pltpu.roll(block, 1, 1)
            up_end = jnp.where(lane == 127, 0.0, up[:, lat - 128:])
            down_end = jnp.where(lane == 0, 0.0, down[:, :128])
            up = jnp.concatenate([up[:, :lat - 128], up_end], axis=1)
            down = jnp.concatenate([down_end, down[:, 128:]], axis=1)
            return HALF * (up - down)

        height = source[0, here, :]
        along_lon, along_lat = lon_diff(0, height), lat_diff(height)
        if rest:
            zonal, merid = source[1, here, :], source[2, here, :]
            new = less(height, lon_diff(1, zonal) + lat_diff(merid))
            target[1, here, :] = less(zonal, along_lon - cor_c * merid)
            target[2, here, :] = less(merid, along_lat + cor_c * zonal)
        else:
            new = height
            target[1, here, :] = less(0.0, along_lon)
            target[2, here, :] = less(0.0, along_lat)
        target[0, here, :] = new if extra is None else new + extra[here, :]


def fold(values):
    values = values + pltpu.roll(values, 64, 1)
    return values + pltpu.roll(values, 32, 1)


def pack_rows(rows):
    lane = lax.broadcasted_iota(jnp.int32, (1, 128), 1) // 32
    packed = jnp.zeros((1, 128), jnp.float32)
    for k, row in enumerate(rows):
        packed = jnp.where(lane == k, fold(row), packed)
    return packed


def unpack_rows(total, number):
    lane = lax.broadcasted_iota(jnp.int32, (1, 128), 1) // 32
    return [
        jnp.sum(jnp.where(lane == k, total, 0.0), axis=1, keepdims=True) for k in range(number)
    ]


def lane_sum(values):
    total = values[:, :128]
    for k in range(128, values.shape[1], 128):
        total = total + values[:, k:k + 128]
    return total


def remote_count(ens, lat, nobs):
    return 4 + (ens - 1) * len(SHARES)


def side_rows():
    return [(n, k) for n in reversed(range(STEPS)) for k in range(n + 1)]


def kernel(
    ens, lon, control_hbm, direction_hbm, residual_hbm, perturb_hbm, localize_hbm, cell_hbm,
    slot_hbm, weight_hbm, consts_hbm,
    control, residual, direction, image, scalars,
    localize, perturb, cell, slot, weight, consts,
    high, low, split, onehot, state0, state1, state2, state3, heights, observed, arrived,
    spread, forcing, near, near_in, mass, mass_in, tiles, tile,
    load_sem, send_sem, recv_sem, tile_send, tile_recv,
):
    me_e, me_l = lax.axis_index("ens"), lax.axis_index("lon")
    members, cols, lat = direction.shape
    nobs = cell.shape[1]
    wide = state0.shape[1]
    stacked = members * cols
    slots_cols = STEPS * cols
    blocks = [pl.ds(k, BLOCK) for k in range(0, lat, BLOCK)]
    cuts = [nobs * share // SHARES[-1] for share in SHARES]
    chunks = [pl.ds(start, stop - start) for start, stop in zip(cuts, cuts[1:])]
    panels = range(lat // 128)

    def wrap(value, size):
        return jnp.where(value >= size, value - size, value)

    left_dev = (me_e, wrap(me_l + lon - 1, lon))
    right_dev = (me_e, wrap(me_l + 1, lon))

    load_ids = itertools.count()

    def load(src, dst):
        copy = pltpu.make_async_copy(src, dst, load_sem.at[next(load_ids)])
        copy.start()
        return copy

    load_obs = [load(cell_hbm, cell), load(slot_hbm, slot), load(weight_hbm, weight)]
    load_d = load(direction_hbm, direction)
    load_l = [load(localize_hbm.at[at, :], localize.at[at, :]) for at in blocks[:2]]
    load_p = load(perturb_hbm, perturb)
    load_l += [load(localize_hbm.at[at, :], localize.at[at, :]) for at in blocks[2:]]
    load_c = load(consts_hbm, consts)
    load_r = load(residual_hbm, residual)
    load_v = load(control_hbm, control)

    barrier = pltpu.get_barrier_semaphore()
    ids = itertools.count()

    def remote(src, dst, device):
        k = next(ids)
        return pltpu.make_async_remote_copy(
            src_ref=src, dst_ref=dst, send_sem=send_sem.at[k], recv_sem=recv_sem.at[k],
            device_id=device, device_id_type=MESH,
        )

    def each_peer(act):
        for e in range(ens):
            peer_e = wrap(me_e + e, ens)

            def visit(l, carry):
                act(e * lon + l - 1, (peer_e, wrap(me_l + l, lon)))
                return carry

            lax.fori_loop(0 if e else 1, lon, visit, 0, unroll=True)

    each_peer(lambda index, device: pl.semaphore_signal(
        barrier, inc=1, device_id=device, device_id_type=MESH
    ))

    for copy in load_obs:
        copy.wait()
    rows = (cell[...] // cols).reshape(nobs // 128, 128)
    rows = jnp.concatenate([rows] * (128 * 128 // nobs), axis=0).T
    lanes = lax.broadcasted_iota(jnp.int32, (16, 128), 1).astype(jnp.int16)
    one, zero = jnp.ones((16, 128), jnp.bfloat16), jnp.zeros((16, 128), jnp.bfloat16)

    def mark(groups):
        for group in groups:
            for s in range(0, 128, 16):
                row = jnp.broadcast_to(rows[s:s + 16, group:group + 1], (16, 128))
                row = row.astype(jnp.int16)
                for j in panels:
                    hit = row == lanes + jnp.int16(128 * j)
                    onehot[j, pl.ds(128 * group + s, 16), :] = jnp.where(hit, one, zero)

    groups = nobs // 128
    mark(range(0, groups // 2))

    def panel(ref, at, which=panels):
        return jnp.concatenate([ref[j, at, :] for j in which], axis=1)

    def store_panels(ref, at, values):
        for j in panels:
            ref[j, at, :] = values[:, 128 * j:128 * j + 128]

    load_d.wait()
    d_high, d_low = split_bf16(direction[...].reshape(stacked, lat))

    edge = 2 * STEPS
    own = pl.ds(HALO, cols)
    first, last = pl.ds(HALO, edge), pl.ds(HALO + cols - edge, edge)
    before, after = pl.ds(HALO - edge, edge), pl.ds(HALO + cols, edge)
    d_both = jnp.concatenate([d_high, d_low], axis=0)
    mark(range(groups // 2, groups * 3 // 4))
    for k, at in enumerate(blocks):
        if k % 2 == 0:
            load_l[k].wait()
            load_l[k + 1].wait()
            if k == 0:
                load_p.wait()
        l_high, l_low = split_bf16(localize[at, :])
        store_panels(high, at, l_high)
        store_panels(low, at, l_low)
        both = dot(d_both, l_high, NT)
        local = both[:stacked] + both[stacked:] + dot(d_high, l_low, NT)
        for c in range(3):
            total = None
            for m in range(members):
                term = perturb[m, c, :, at].astype(jnp.float32) * local[m * cols:(m + 1) * cols]
                total = term if total is None else total + term
            state0[c, own, at] = total
        mark(range(groups * (12 + k) // 16, groups * (13 + k) // 16))
    def keys(at):
        cells, slots = cell[:, at], slot[:, at]
        return slots * cols + (cells - cells // cols * cols)

    def scattered(hit, values):
        v_high = values.astype(jnp.bfloat16).astype(jnp.float32)
        return jnp.concatenate(
            [jnp.where(hit, v_high, 0.0), jnp.where(hit, values - v_high, 0.0)], axis=0
        ).astype(jnp.bfloat16)

    load_c.wait()
    load_r.wait()
    states = (state0, state1, state2, state3)

    def keep(n, starts):
        for start in starts:
            value = states[n + 1][0, pl.ds(start, 8), :]
            v_high = value.astype(jnp.bfloat16).astype(jnp.float32)
            row = n * cols + start - HALO
            heights[pl.ds(row, 8), :] = v_high
            heights[pl.ds(slots_cols + row, 8), :] = value - v_high

    mid = range(HALO + 8, HALO + cols - 8, 8)
    def side_ids(width):
        row = lax.broadcasted_iota(jnp.int32, (16, 128), 0)
        result = jnp.full((16, 128), -1, jnp.int32)
        for k, (n, dist) in enumerate(side_rows()):
            result = jnp.where(row == k, n * cols + dist, result)
            result = jnp.where(row == 8 + k, n * cols + cols - 1 - n + dist, result)
        return jnp.concatenate([result] * (width // 128), axis=1)


    def before_halo():
        for n in range(STEPS):
            starts = range(HALO, HALO + cols, 8) if n < STEPS - 1 else mid
            linear_step(states[n], states[n + 1], 1, consts, starts, HALO, HALO + cols)
            keep(n, mid)

        left = scattered(side_ids(nobs) == keys(pl.ds(0, nobs)), weight[...])
        both = dot(left, panel(onehot, pl.ds(0, nobs)), NN)
        mass[...] = (both[:16] + both[16:]).reshape(2, 8, lat)

    is_first = (me_l == 0) & (me_e == 0)
    pl.when(is_first)(before_halo)

    pl.semaphore_wait(barrier, ens * lon - 1)
    f_copies = [
        remote(state0.at[:, first], state0.at[:, after], left_dev),
        remote(state0.at[:, last], state0.at[:, before], right_dev),
    ]
    for copy in f_copies:
        copy.start()

    pl.when(jnp.logical_not(is_first))(before_halo)
    norm_old = jnp.zeros((8, 128), jnp.float32)
    for at in blocks:
        value = residual[:, :, at]
        norm_old += lane_sum((value * value).reshape(stacked // 8, 8, BLOCK).sum(axis=0))

    used = pl.ds(0, len(side_rows()))
    m_copies = [
        remote(mass.at[0, used], mass_in.at[1, used], left_dev),
        remote(mass.at[1, used], mass_in.at[0, used], right_dev),
    ]
    for copy in m_copies:
        copy.start()

    is_end = me_l == 0
    mid_cols = cols - 16
    key_ids = lax.broadcasted_iota(jnp.int32, (slots_cols, nobs), 0)

    def gather(ranges, key_of, done):
        rows = [
            pl.ds(h * slots_cols + n * cols + start, size)
            for h in range(2) for n in range(STEPS) for start, size in ranges
        ]
        table = jnp.concatenate([heights[row, :] for row in rows], axis=0).astype(jnp.bfloat16)
        count = table.shape[0] // 2

        def finish(k, both):
            at = chunks[k]
            slots, key = slot[:, at], keys(at)
            key = key_of(slots, key - slots * cols)
            both = both[:count] + both[count:]
            both = jnp.where(key_ids[:count, :both.shape[1]] == key, both, 0.0)
            done(k, at, jnp.sum(both, axis=0, keepdims=True))

        ahead = None
        for k, at in enumerate(chunks):
            both = dot(table, panel(onehot, at), NT)
            if ahead is not None:
                finish(k - 1, ahead)
            ahead = both
        finish(len(chunks) - 1, ahead)

    def mid_key(slots, col):
        inside = (col >= 8) & (col < cols - 8) & (slots < STEPS)
        return jnp.where(inside, slots * mid_cols + col - 8, -1)

    def edge_key(slots, col):
        inside = (col >= 8) & (col < cols - 8)
        place = jnp.where(col < 8, col, col - mid_cols)
        return jnp.where(inside | (slots >= STEPS), -1, slots * 16 + place)

    @pl.when(is_end)
    def _():
        def done(k, at, values):
            observed[:, at] = values

        gather([(8, mid_cols)], mid_key, done)

    for copy in f_copies:
        copy.wait_recv()
    ends = (0, HALO, HALO + cols - 8, HALO + cols)
    for n in range(STEPS):
        linear_step(states[n], states[n + 1], 1, consts, ends, 0, wide)
        keep(n, (HALO, HALO + cols - 8))
    tall = 2 if ens % 2 == 0 else 1
    broad = ens // tall
    me_a = me_e // broad
    me_b = me_e - me_a * broad
    straight = [(0, j) for j in range(1, broad)] + [(i, 0) for i in range(1, tall)]
    slanted = [(i, j) for i in range(1, tall) for j in range(1, broad)]
    peers = [
        (wrap(me_a + i, tall) * broad + wrap(me_b + j, broad), me_l)
        for i, j in straight + slanted
    ]
    for k, (n, dist) in enumerate(side_rows()):
        near[0, pl.ds(k, 1), :] = states[n + 1][0, pl.ds(HALO - 1 - n + dist, 1), :]
        near[1, pl.ds(k, 1), :] = states[n + 1][0, pl.ds(HALO + cols + dist, 1), :]
    n_copies = [
        remote(near.at[:, used], near_in.at[j, :, used], peer) for j, peer in enumerate(peers)
    ]

    for copy in n_copies[:len(straight)]:
        copy.start()

    sums = {
        (j, k): remote(observed.at[:, at], arrived.at[j, :, at], peer)
        for k, at in enumerate(chunks) for j, peer in enumerate(peers)
    }

    def send(k):
        for j in range(ens - 1):
            sums[j, k].start()
        if k == 0:
            for copy in n_copies[len(straight):]:
                copy.start()

    @pl.when(is_end)
    def _():
        def done(k, at, values):
            observed[:, at] += values
            send(k)

        gather([(0, 8), (cols - 8, 8)], edge_key, done)

    @pl.when(jnp.logical_not(is_end))
    def _():
        def done(k, at, values):
            observed[:, at] = values
            send(k)

        gather([(0, cols)], lambda slots, col: slots * cols + col, done)

    for k, at in enumerate(chunks):
        for j in range(ens - 1):
            sums[j, k].wait_recv()
        total = observed[:, at]
        for j in range(ens - 1):
            total = total + arrived[j, :, at]
        left = scattered(key_ids[:, :total.shape[1]] == keys(at), weight[:, at] * total)
        both = dot(left, panel(onehot, at), NN)
        both = both[:slots_cols] + both[slots_cols:]
        if k == 0:
            spread[...] = both
        elif k < len(chunks) - 1:
            spread[...] += both
        else:
            both = spread[...] + both
            for s in range(STEPS):
                forcing[s, own, :] = both[s * cols:(s + 1) * cols]

    for copy in m_copies + n_copies:
        copy.wait_recv()
    for side in range(2):
        total = near[side]
        for j in range(ens - 1):
            total = total + near_in[j, side]
        total = total * mass_in[side]
        for k, (n, dist) in enumerate(side_rows()):
            row = HALO + cols + dist if side else HALO - 1 - n + dist
            forcing[n, pl.ds(row, 1), :] = total[k:k + 1]
    every = range(0, wide, 8)
    inner = range(HALO, HALO + cols, 8)
    linear_step(forcing.at[pl.ds(2, 1)], state1, -1, consts, every, 0, wide, False, forcing.at[1])
    linear_step(state1, state2, -1, consts, every, 0, wide, True, forcing.at[0])
    linear_step(state2, state3, -1, consts, inner, 0, wide)

    for m in range(members):
        total = None
        for c in range(3):
            term = perturb[m, c].astype(jnp.float32) * state3[c, own, :]
            total = term if total is None else total + term
        p_high, p_low = split_bf16(total)
        store_panels(split, pl.ds(m * cols, cols), p_high)
        store_panels(split, pl.ds(stacked + m * cols, cols), p_low)

    p_both = panel(split, pl.ds(0, 2 * stacked))
    sums_new = [norm_old] + [jnp.zeros((8, 128), jnp.float32)] * 3
    for k, at in enumerate(blocks):
        pair = range(k * BLOCK // 128, (k + 1) * BLOCK // 128)
        both = dot(p_both, panel(high, pl.ds(0, lat), pair), NN)
        back = both[:stacked] + both[stacked:]
        back += dot(p_both[:stacked], panel(low, pl.ds(0, lat), pair), NN)
        d = direction[:, :, at].reshape(stacked, BLOCK)
        r = residual[:, :, at].reshape(stacked, BLOCK)
        img = d + back
        image[:, :, at] = img.reshape(members, cols, BLOCK)
        for j, term in enumerate((d * img, r * img, img * img)):
            sums_new[j + 1] += lane_sum(term.reshape(stacked // 8, 8, BLOCK).sum(axis=0))

    tile[...] = pack_rows([jnp.sum(value, axis=0, keepdims=True) for value in sums_new])

    def tell(index, device):
        pltpu.make_async_remote_copy(
            src_ref=tile, dst_ref=tiles.at[index], send_sem=tile_send, recv_sem=tile_recv,
            device_id=device, device_id_type=MESH,
        ).start()

    each_peer(tell)
    load_v.wait()
    for copy in f_copies + m_copies + n_copies + list(sums.values()):
        copy.wait_send()
    everything = pltpu.make_async_remote_copy(
        src_ref=tiles, dst_ref=tiles, send_sem=tile_send, recv_sem=tile_recv,
        device_id=right_dev, device_id_type=MESH,
    )
    everything.wait_send()
    everything.wait_recv()
    norm_old, curvature, cross_term, square = unpack_rows(
        jnp.sum(tiles[...], axis=0) + tile[...], 4
    )
    step_size = norm_old / curvature
    norm_new = norm_old - 2.0 * step_size * cross_term + step_size * step_size * square
    scalars[pl.ds(0, 1), :] = jnp.broadcast_to(step_size, (1, 128))
    scalars[pl.ds(1, 1), :] = jnp.broadcast_to(norm_new / norm_old, (1, 128))


def update(
    control, residual, direction, image, scalars, control_out, residual_out, direction_out,
    control_new, residual_new, direction_new, sem,
):
    step_size, ratio = scalars[pl.ds(0, 1), pl.ds(0, 1)], scalars[pl.ds(1, 1), pl.ds(0, 1)]
    ids = itertools.count()
    copies = []

    def send(src, dst, at):
        copies.append(pltpu.make_async_copy(src.at[at], dst.at[at], sem.at[next(ids)]))
        copies[-1].start()

    members, cols = control.shape[:2]
    for m in range(members):
        for h in range(2):
            at = (m, pl.ds(h * cols // 2, cols // 2))
            d = direction[at]
            new = residual[at] - step_size * image[at]
            residual_new[at] = new
            direction_new[at] = new + ratio * d
            control_new[at] = control[at] + step_size * d
            send(residual_new, residual_out, at)
            send(direction_new, direction_out, at)
            send(control_new, control_out, at)
    for copy in copies:
        copy.wait()


def body(ens, lon, control, residual, direction, ens_perturb, localize, obs_cell, obs_slot, obs_weight):
    flip = functools.partial(jnp.swapaxes, axis1=-1, axis2=-2)
    control, residual, direction, ens_perturb = map(flip, (control, residual, direction, ens_perturb))
    members, cols, lat = direction.shape
    nobs = obs_cell.shape[0]
    count = ens * lon
    wide = cols + 2 * HALO
    f32, bf16, i32 = jnp.float32, jnp.bfloat16, jnp.int32
    hbm = pl.BlockSpec(memory_space=pltpu.HBM)
    dma = pltpu.SemaphoreType.DMA
    field = pltpu.VMEM((members, cols, lat), f32)
    vmem = pl.BlockSpec(memory_space=pltpu.VMEM)
    copies = remote_count(ens, lat, nobs)
    outs = pl.pallas_call(
        functools.partial(kernel, ens, lon),
        out_shape=(field, field, field, field, pltpu.VMEM((8, 128), f32)),
        in_specs=[hbm] * 9,
        out_specs=(vmem,) * 5,
        scratch_shapes=[
            pltpu.VMEM((lat, lat), f32),
            pltpu.VMEM((members, 3, cols, lat), bf16),
            pltpu.VMEM((1, nobs), i32),
            pltpu.VMEM((1, nobs), i32),
            pltpu.VMEM((1, nobs), f32),
            pltpu.VMEM((2, 8, lat), f32),
            pltpu.VMEM((lat // 128, lat, 128), bf16),
            pltpu.VMEM((lat // 128, lat, 128), bf16),
            pltpu.VMEM((lat // 128, 2 * members * cols, 128), bf16),
            pltpu.VMEM((lat // 128, nobs, 128), bf16),
            pltpu.VMEM((3, wide, lat), f32),
            pltpu.VMEM((3, wide, lat), f32),
            pltpu.VMEM((3, wide, lat), f32),
            pltpu.VMEM((3, wide, lat), f32),
            pltpu.VMEM((2 * STEPS * cols, lat), f32),
            pltpu.VMEM((1, nobs), f32),
            pltpu.VMEM((max(ens - 1, 1), 1, nobs), f32),
            pltpu.VMEM((STEPS * cols, lat), f32),
            pltpu.VMEM((STEPS, wide, lat), f32),
            pltpu.VMEM((2, 8, lat), f32),
            pltpu.VMEM((max(ens - 1, 1), 2, 8, lat), f32),
            pltpu.VMEM((2, 8, lat), f32),
            pltpu.VMEM((2, 8, lat), f32),
            pltpu.VMEM((count - 1, 1, 128), f32),
            pltpu.VMEM((1, 128), f32),
            dma((8 + lat // BLOCK,)), dma((copies,)), dma((copies,)),
            dma, dma,
        ],
        compiler_params=pltpu.CompilerParams(
            collective_id=0, has_side_effects=True, vmem_limit_bytes=61 * 1024 * 1024
        ),
    )(
        control, direction, residual, ens_perturb, localize,
        obs_cell.reshape(1, nobs), obs_slot.reshape(1, nobs), obs_weight.reshape(1, nobs),
        jnp.asarray(grid_constants(lat)),
    )
    outs = pl.pallas_call(
        update,
        out_shape=[jax.ShapeDtypeStruct((members, cols, lat), f32)] * 3,
        in_specs=[vmem] * 5,
        out_specs=[hbm] * 3,
        scratch_shapes=[pltpu.VMEM((members, cols, lat), f32)] * 3 + [dma((6 * members,))],
        compiler_params=pltpu.CompilerParams(vmem_limit_bytes=8 * 1024 * 1024),
    )(*outs)
    return tuple(map(flip, outs))


def solution(mesh):
    fields = P("ens", None, "lon")
    in_specs = (fields, fields, fields, P("ens", None, None, "lon"), P(), P("lon"), P("lon"), P("lon"))
    ens, lon = mesh.shape["ens"], mesh.shape["lon"]
    return jax.shard_map(
        functools.partial(body, ens, lon), mesh=mesh, in_specs=in_specs,
        out_specs=(fields, fields, fields), check_vma=False,
    )
```

```python
import functools
import itertools

import numpy as np
import jax
import jax.numpy as jnp
from jax import lax
from jax.experimental import pallas as pl
from jax.experimental.pallas import tpu as pltpu
from jax.sharding import PartitionSpec as P

STEPS = 3
HALO = 8
HALF = 0.5 * 0.35
SHARES = (0, 4, 8, 13, 16)
BLOCK = 256
MESH = pl.DeviceIdType.MESH
NT = (((1,), (1,)), ((), ()))
NN = (((1,), (0,)), ((), ()))


def split_bf16(values):
    high = values.astype(jnp.bfloat16)
    low = (values - high.astype(jnp.float32)).astype(jnp.bfloat16)
    return high, low


def dot(left, right, dims):
    return lax.dot_general(left, right, dims, preferred_element_type=jnp.float32)


def grid_constants(lat):
    phi = np.pi * (-1.0 / 3.0 + 2.0 / 3.0 * (np.arange(lat) + 0.5) / lat)
    rows = np.stack([HALF / np.cos(phi), 0.2 * np.sin(phi)])
    return np.ascontiguousarray(np.broadcast_to(rows[:, None], (2, 8, lat))).astype(np.float32)


def linear_step(source, target, sign, consts, blocks, low_end, high_end, rest=True, extra=None):
    lat = source.shape[2]
    lon_c, cor_c = consts[0], consts[1]
    lane = lax.broadcasted_iota(jnp.int32, (8, 128), 1)

    def less(value, term):
        return value - term if sign > 0 else value + term

    for start in blocks:
        here = pl.ds(start, 8)

        def lon_diff(comp, block):
            if start + 8 == high_end:
                east = pltpu.roll(block, 7, 0)
            else:
                east = source[comp, pl.ds(start + 1, 8), :]
            if start == low_end:
                west = pltpu.roll(block, 1, 0)
            else:
                west = source[comp, pl.ds(start - 1, 8), :]
            return lon_c * (east - west)

        def lat_diff(block):
            up, down = pltpu.roll(block, lat - 1, 1), pltpu.roll(block, 1, 1)
            up_end = jnp.where(lane == 127, 0.0, up[:, lat - 128:])
            down_end = jnp.where(lane == 0, 0.0, down[:, :128])
            up = jnp.concatenate([up[:, :lat - 128], up_end], axis=1)
            down = jnp.concatenate([down_end, down[:, 128:]], axis=1)
            return HALF * (up - down)

        height = source[0, here, :]
        along_lon, along_lat = lon_diff(0, height), lat_diff(height)
        if rest:
            zonal, merid = source[1, here, :], source[2, here, :]
            new = less(height, lon_diff(1, zonal) + lat_diff(merid))
            target[1, here, :] = less(zonal, along_lon - cor_c * merid)
            target[2, here, :] = less(merid, along_lat + cor_c * zonal)
        else:
            new = height
            target[1, here, :] = less(0.0, along_lon)
            target[2, here, :] = less(0.0, along_lat)
        target[0, here, :] = new if extra is None else new + extra[here, :]


def fold(values):
    values = values + pltpu.roll(values, 64, 1)
    return values + pltpu.roll(values, 32, 1)


def pack_rows(rows):
    lane = lax.broadcasted_iota(jnp.int32, (1, 128), 1) // 32
    packed = jnp.zeros((1, 128), jnp.float32)
    for k, row in enumerate(rows):
        packed = jnp.where(lane == k, fold(row), packed)
    return packed


def unpack_rows(total, number):
    lane = lax.broadcasted_iota(jnp.int32, (1, 128), 1) // 32
    return [
        jnp.sum(jnp.where(lane == k, total, 0.0), axis=1, keepdims=True) for k in range(number)
    ]


def lane_sum(values):
    total = values[:, :128]
    for k in range(128, values.shape[1], 128):
        total = total + values[:, k:k + 128]
    return total


LEFT_COPY, RIGHT_COPY, MASS_COPY, NEAR_COPY, LATE_COPY, SUM_COPY = range(6)


def side_rows():
    return [(n, k) for n in reversed(range(STEPS)) for k in range(n + 1)]


def kernel(
    ens, lon, control_hbm, direction_hbm, residual_hbm, perturb_hbm, localize_hbm, cell_hbm,
    slot_hbm, weight_hbm, consts_hbm,
    control, residual, direction, image, scalars,
    localize, perturb, cell, slot, weight, consts,
    high, low, split, onehot, state0, state1, state2, state3, heights, observed, arrived,
    spread, forcing, near, near_in, mass, mass_in, tiles, tile,
    load_sem, send_sem, recv_sem, tile_send, tile_recv,
):
    me_e, me_l = lax.axis_index("ens"), lax.axis_index("lon")
    members, cols, lat = direction.shape
    nobs = cell.shape[1]
    wide = state0.shape[1]
    stacked = members * cols
    slots_cols = STEPS * cols
    blocks = [pl.ds(k, BLOCK) for k in range(0, lat, BLOCK)]
    cuts = [nobs * share // SHARES[-1] for share in SHARES]
    chunks = [pl.ds(start, stop - start) for start, stop in zip(cuts, cuts[1:])]
    panels = range(lat // 128)

    def wrap(value, size):
        return jnp.where(value >= size, value - size, value)

    left_dev = (me_e, wrap(me_l + lon - 1, lon))
    right_dev = (me_e, wrap(me_l + 1, lon))

    load_ids = itertools.count()

    def load(src, dst):
        copy = pltpu.make_async_copy(src, dst, load_sem.at[next(load_ids)])
        copy.start()
        return copy

    load_obs = [load(cell_hbm, cell), load(slot_hbm, slot), load(weight_hbm, weight)]
    load_d = load(direction_hbm, direction)
    halves = [pl.ds(k, lat // 2) for k in (0, lat // 2)]
    load_l = [load(localize_hbm.at[halves[0]], localize.at[halves[0]])]
    load_p = load(perturb_hbm, perturb)
    load_l.append(load(localize_hbm.at[halves[1]], localize.at[halves[1]]))
    load_c = load(consts_hbm, consts)
    load_r = load(residual_hbm, residual)
    load_v = load(control_hbm, control)

    barrier = pltpu.get_barrier_semaphore()

    def remote(src, dst, device, kind, arrival):
        return pltpu.make_async_remote_copy(
            src_ref=src, dst_ref=dst, send_sem=send_sem.at[kind], recv_sem=recv_sem.at[arrival],
            device_id=device, device_id_type=MESH,
        )

    def all_of(ref, kind, arrival):
        return remote(ref, ref, right_dev, kind, arrival)

    order = sorted(range(lon), key=lambda l: (l == 0, min(l, lon - l), l))

    def each_peer(act):
        peers_e = [wrap(me_e + e, ens) for e in range(ens)]
        for l in order:
            peer_l = wrap(me_l + l, lon)
            for e in range(ens):
                if e or l:
                    act(e * lon + l - 1, (peers_e[e], peer_l))

    each_peer(lambda index, device: pl.semaphore_signal(
        barrier, inc=1, device_id=device, device_id_type=MESH
    ))

    for copy in load_obs:
        copy.wait()
    rows = (cell[...] // cols).reshape(nobs // 128, 128)
    rows = jnp.concatenate([rows] * (128 * 128 // nobs), axis=0).T
    lanes = lax.broadcasted_iota(jnp.int32, (16, 128), 1).astype(jnp.int16)
    one, zero = jnp.ones((16, 128), jnp.bfloat16), jnp.zeros((16, 128), jnp.bfloat16)

    def mark(groups):
        for group in groups:
            for s in range(0, 128, 16):
                row = jnp.broadcast_to(rows[s:s + 16, group:group + 1], (16, 128))
                row = row.astype(jnp.int16)
                for j in panels:
                    hit = row == lanes + jnp.int16(128 * j)
                    onehot[j, pl.ds(128 * group + s, 16), :] = jnp.where(hit, one, zero)

    groups = nobs // 128
    mark(range(0, groups // 2))

    def panel(ref, at, which=panels):
        return jnp.concatenate([ref[j, at, :] for j in which], axis=1)

    def store_panels(ref, at, values):
        for j in panels:
            ref[j, at, :] = values[:, 128 * j:128 * j + 128]

    load_d.wait()
    d_high, d_low = split_bf16(direction[...].reshape(stacked, lat))

    edge = 2 * STEPS
    own = pl.ds(HALO, cols)
    first, last = pl.ds(HALO, edge), pl.ds(HALO + cols - edge, edge)
    before, after = pl.ds(HALO - edge, edge), pl.ds(HALO + cols, edge)
    d_both = jnp.concatenate([d_high, d_low], axis=0)
    mark(range(groups // 2, groups * 3 // 4))
    for k, at in enumerate(blocks):
        if k % (len(blocks) // 2) == 0:
            load_l[k // (len(blocks) // 2)].wait()
            if k == 0:
                load_p.wait()
        l_high, l_low = split_bf16(localize[at, :])
        store_panels(high, at, l_high)
        store_panels(low, at, l_low)
        both = dot(d_both, l_high, NT)
        local = both[:stacked] + both[stacked:] + dot(d_high, l_low, NT)
        for c in range(3):
            total = None
            for m in range(members):
                term = perturb[m, c, :, at].astype(jnp.float32) * local[m * cols:(m + 1) * cols]
                total = term if total is None else total + term
            state0[c, own, at] = total
        mark(range(groups * (12 + k) // 16, groups * (13 + k) // 16))
    def keys(at):
        cells, slots = cell[:, at], slot[:, at]
        return slots * cols + (cells - cells // cols * cols)

    def scattered(hit, values):
        v_high = values.astype(jnp.bfloat16).astype(jnp.float32)
        return jnp.concatenate(
            [jnp.where(hit, v_high, 0.0), jnp.where(hit, values - v_high, 0.0)], axis=0
        ).astype(jnp.bfloat16)

    load_c.wait()
    load_r.wait()
    states = (state0, state1, state2, state3)

    def keep(n, starts):
        for start in starts:
            value = states[n + 1][0, pl.ds(start, 8), :]
            v_high = value.astype(jnp.bfloat16).astype(jnp.float32)
            row = n * cols + start - HALO
            heights[pl.ds(row, 8), :] = v_high
            heights[pl.ds(slots_cols + row, 8), :] = value - v_high

    inner = range(HALO, HALO + cols, 8)
    def side_ids(width):
        row = lax.broadcasted_iota(jnp.int32, (16, 128), 0)
        result = jnp.full((16, 128), -1, jnp.int32)
        for k, (n, dist) in enumerate(side_rows()):
            result = jnp.where(row == k, n * cols + dist, result)
            result = jnp.where(row == 8 + k, n * cols + cols - 1 - n + dist, result)
        return jnp.concatenate([result] * (width // 128), axis=1)


    def before_halo():
        for n in range(STEPS):
            linear_step(states[n], states[n + 1], 1, consts, inner, HALO, HALO + cols)
            keep(n, inner)

        left = scattered(side_ids(nobs) == keys(pl.ds(0, nobs)), weight[...])
        both = dot(left, panel(onehot, pl.ds(0, nobs)), NN)
        mass[...] = (both[:16] + both[16:]).reshape(2, 8, lat)

    is_first = (me_l == 0) & (me_e == 0)
    pl.when(is_first)(before_halo)

    pl.semaphore_wait(barrier, ens * lon - 1)
    f_copies = [
        remote(state0.at[:, first], state0.at[:, after], left_dev, LEFT_COPY, 0),
        remote(state0.at[:, last], state0.at[:, before], right_dev, RIGHT_COPY, 1),
    ]
    for copy in f_copies:
        copy.start()

    pl.when(jnp.logical_not(is_first))(before_halo)
    norm_old = jnp.zeros((8, 128), jnp.float32)
    for at in blocks:
        value = residual[:, :, at]
        norm_old += lane_sum((value * value).reshape(stacked // 8, 8, BLOCK).sum(axis=0))

    used = pl.ds(0, len(side_rows()))
    m_copies = [
        remote(mass.at[0, used], mass_in.at[1, used], left_dev, MASS_COPY, 2),
        remote(mass.at[1, used], mass_in.at[0, used], right_dev, MASS_COPY, 2),
    ]
    for copy in m_copies:
        copy.start()

    is_left, is_right = me_l == 0, me_l == lon - 1
    is_end = is_left | is_right
    key_ids = lax.broadcasted_iota(jnp.int32, (slots_cols, nobs), 0)
    tall = 2 if ens % 2 == 0 else 1
    broad = ens // tall
    me_a = me_e // broad
    me_b = me_e - me_a * broad
    straight = [(0, j) for j in range(1, broad)] + [(i, 0) for i in range(1, tall)]
    slanted = [(i, j) for i in range(1, tall) for j in range(1, broad)]
    peers = [
        (wrap(me_a + i, tall) * broad + wrap(me_b + j, broad), me_l)
        for i, j in straight + slanted
    ]
    n_copies = [
        [
            remote(near.at[part, used], near_in.at[j, part, used], peer, kind, arrival)
            for part, kind, arrival in ((0, NEAR_COPY, 3), (1, NEAR_COPY, 3), (2, LATE_COPY, 4))
        ]
        for j, peer in enumerate(peers)
    ]
    sums = {
        (j, k): remote(observed.at[:, at], arrived.at[j, :, at], peer, SUM_COPY, 5 + k)
        for k, at in enumerate(chunks) for j, peer in enumerate(peers)
    }
    far = (is_left, is_right)
    own_edge = (
        lambda n, dist: HALO + dist,
        lambda n, dist: HALO + cols - 1 - n + dist,
    )
    beyond = (
        lambda n, dist: HALO - 1 - n + dist,
        lambda n, dist: HALO + cols + dist,
    )

    def outer(side):
        starts = (HALO + cols - 8, HALO + cols) if side else (0, HALO)
        f_copies[1 - side].wait_recv()
        for n in range(STEPS):
            linear_step(states[n], states[n + 1], 1, consts, starts, 0, wide)
            keep(n, starts[:1] if side else starts[1:])
        for k, (n, dist) in enumerate(side_rows()):
            near[side, pl.ds(k, 1), :] = states[n + 1][0, pl.ds(beyond[side](n, dist), 1), :]

    def outer_late(side):
        outer(side)
        for k, (n, dist) in enumerate(side_rows()):
            near[2, pl.ds(k, 1), :] = states[n + 1][0, pl.ds(own_edge[side](n, dist), 1), :]
        for parts in n_copies:
            parts[side].start()
            parts[2].start()

    for side in range(2):
        @pl.when(jnp.logical_not(far[side]))
        def _():
            outer(side)
            for parts in n_copies[:len(straight)]:
                parts[side].start()

    first_own = jnp.where(is_left, 0, -cols)
    last_own = jnp.where(is_right, cols - 1, 2 * cols)

    def gather(which, after_first):
        table = heights[...].astype(jnp.bfloat16)

        def finish(k, both):
            at = chunks[k]
            slots, key = slot[:, at], keys(at)
            col = key - slots * cols
            late = (col <= slots + first_own) | (col >= last_own - slots)
            both = both[:slots_cols] + both[slots_cols:]
            hit = key_ids[:, :both.shape[1]] == jnp.where(late, -1, key)
            observed[:, at] = jnp.sum(jnp.where(hit, both, 0.0), axis=0, keepdims=True)
            for j in range(ens - 1):
                sums[j, k].start()
            if k == 0:
                after_first()

        ahead = None
        for k in which:
            both = dot(table, panel(onehot, chunks[k]), NT)
            if ahead is not None:
                finish(*ahead)
            ahead = (k, both)
        finish(*ahead)

    number = len(chunks)

    def slanted_start(sides):
        for parts in n_copies[len(straight):]:
            for side in sides:
                parts[side].start()

    @pl.when(is_end)
    def _():
        gather(range(number - 1), lambda: None)
        for side in range(2):
            @pl.when(far[side])
            def _():
                slanted_start((1 - side,))
                outer_late(side)
        gather(range(number - 1, number), lambda: None)

    @pl.when(jnp.logical_not(is_end))
    def _():
        gather(range(number), lambda: slanted_start(range(2)))

    for k, at in enumerate(chunks):
        all_of(arrived.at[:, :, at], SUM_COPY, 5 + k).wait_recv()
        total = observed[:, at]
        for j in range(ens - 1):
            total = total + arrived[j, :, at]
        left = scattered(key_ids[:, :total.shape[1]] == keys(at), weight[:, at] * total)
        both = dot(left, panel(onehot, at), NN)
        both = both[:slots_cols] + both[slots_cols:]
        if k == 0:
            spread[...] = both
        elif k < len(chunks) - 1:
            spread[...] += both
        else:
            both = spread[...] + both
            for s in range(STEPS):
                forcing[s, own, :] = both[s * cols:(s + 1) * cols]

    both_sides = pl.ds(0, 2)
    m_all = all_of(mass_in.at[:, used], MASS_COPY, 2)
    n_all = all_of(near_in.at[:, both_sides, used], NEAR_COPY, 3)
    late_all = all_of(near_in.at[:, 2, used], LATE_COPY, 4)
    m_all.wait_recv()
    n_all.wait_recv()

    def summed(part):
        total = near[part]
        for j in range(ens - 1):
            total = total + near_in[j, part]
        return total

    for side in range(2):
        made = summed(side) * mass_in[side]
        for k, (n, dist) in enumerate(side_rows()):
            forcing[n, pl.ds(beyond[side](n, dist), 1), :] = made[k:k + 1]

        @pl.when(far[side])
        def _():
            late_all.wait_recv()
            made = summed(2) * mass[side]
            for k, (n, dist) in enumerate(side_rows()):
                forcing[n, pl.ds(own_edge[side](n, dist), 1), :] = made[k:k + 1]
    every = range(0, wide, 8)
    linear_step(forcing.at[pl.ds(2, 1)], state1, -1, consts, every, 0, wide, False, forcing.at[1])
    linear_step(state1, state2, -1, consts, every, 0, wide, True, forcing.at[0])
    linear_step(state2, state3, -1, consts, inner, 0, wide)

    for m in range(members):
        total = None
        for c in range(3):
            term = perturb[m, c].astype(jnp.float32) * state3[c, own, :]
            total = term if total is None else total + term
        p_high, p_low = split_bf16(total)
        store_panels(split, pl.ds(m * cols, cols), p_high)
        store_panels(split, pl.ds(stacked + m * cols, cols), p_low)

    p_both = panel(split, pl.ds(0, 2 * stacked))
    sums_new = [norm_old] + [jnp.zeros((8, 128), jnp.float32)] * 3
    for k, at in enumerate(blocks):
        pair = range(k * BLOCK // 128, (k + 1) * BLOCK // 128)
        both = dot(p_both, panel(high, pl.ds(0, lat), pair), NN)
        back = both[:stacked] + both[stacked:]
        back += dot(p_both[:stacked], panel(low, pl.ds(0, lat), pair), NN)
        d = direction[:, :, at].reshape(stacked, BLOCK)
        r = residual[:, :, at].reshape(stacked, BLOCK)
        img = d + back
        image[:, :, at] = img.reshape(members, cols, BLOCK)
        for j, term in enumerate((d * img, r * img, img * img)):
            sums_new[j + 1] += lane_sum(term.reshape(stacked // 8, 8, BLOCK).sum(axis=0))

    tile[...] = pack_rows([jnp.sum(value, axis=0, keepdims=True) for value in sums_new])

    def tell(index, device):
        pltpu.make_async_remote_copy(
            src_ref=tile, dst_ref=tiles.at[index], send_sem=tile_send, recv_sem=tile_recv,
            device_id=device, device_id_type=MESH,
        ).start()

    each_peer(tell)
    load_v.wait()
    for copy in f_copies:
        copy.wait_send()
    all_of(arrived, SUM_COPY, 5).wait_send()
    m_all.wait_send()
    n_all.wait_send()
    pl.when(is_end)(late_all.wait_send)
    everything = pltpu.make_async_remote_copy(
        src_ref=tiles, dst_ref=tiles, send_sem=tile_send, recv_sem=tile_recv,
        device_id=right_dev, device_id_type=MESH,
    )
    everything.wait_send()
    everything.wait_recv()
    norm_old, curvature, cross_term, square = unpack_rows(
        jnp.sum(tiles[...], axis=0) + tile[...], 4
    )
    step_size = norm_old / curvature
    norm_new = norm_old - 2.0 * step_size * cross_term + step_size * step_size * square
    scalars[pl.ds(0, 1), :] = jnp.broadcast_to(step_size, (1, 128))
    scalars[pl.ds(1, 1), :] = jnp.broadcast_to(norm_new / norm_old, (1, 128))


def update(
    control, residual, direction, image, scalars, control_out, residual_out, direction_out,
    control_new, residual_new, direction_new, sem,
):
    step_size, ratio = scalars[pl.ds(0, 1), pl.ds(0, 1)], scalars[pl.ds(1, 1), pl.ds(0, 1)]

    def copy(which, src, dst, *at):
        part = (src.at[at], dst.at[at]) if at else (src, dst)
        return pltpu.make_async_copy(*part, sem.at[which])

    pairs = (
        (residual_new, residual_out), (direction_new, direction_out), (control_new, control_out)
    )
    members, cols = control.shape[:2]
    for m in range(members):
        for h in range(2):
            at = (m, pl.ds(h * cols // 2, cols // 2))
            d = direction[at]
            new = residual[at] - step_size * image[at]
            residual_new[at] = new
            direction_new[at] = new + ratio * d
            control_new[at] = control[at] + step_size * d
            for which, pair in enumerate(pairs):
                copy(which, *pair, *at).start()
    for which, pair in enumerate(pairs):
        copy(which, *pair).wait()


def body(ens, lon, control, residual, direction, ens_perturb, localize, obs_cell, obs_slot, obs_weight):
    flip = functools.partial(jnp.swapaxes, axis1=-1, axis2=-2)
    control, residual, direction, ens_perturb = map(flip, (control, residual, direction, ens_perturb))
    members, cols, lat = direction.shape
    nobs = obs_cell.shape[0]
    count = ens * lon
    wide = cols + 2 * HALO
    f32, bf16, i32 = jnp.float32, jnp.bfloat16, jnp.int32
    hbm = pl.BlockSpec(memory_space=pltpu.HBM)
    dma = pltpu.SemaphoreType.DMA
    field = pltpu.VMEM((members, cols, lat), f32)
    vmem = pl.BlockSpec(memory_space=pltpu.VMEM)
    outs = pl.pallas_call(
        functools.partial(kernel, ens, lon),
        out_shape=(field, field, field, field, pltpu.VMEM((8, 128), f32)),
        in_specs=[hbm] * 9,
        out_specs=(vmem,) * 5,
        scratch_shapes=[
            pltpu.VMEM((lat, lat), f32),
            pltpu.VMEM((members, 3, cols, lat), bf16),
            pltpu.VMEM((1, nobs), i32),
            pltpu.VMEM((1, nobs), i32),
            pltpu.VMEM((1, nobs), f32),
            pltpu.VMEM((2, 8, lat), f32),
            pltpu.VMEM((lat // 128, lat, 128), bf16),
            pltpu.VMEM((lat // 128, lat, 128), bf16),
            pltpu.VMEM((lat // 128, 2 * members * cols, 128), bf16),
            pltpu.VMEM((lat // 128, nobs, 128), bf16),
            pltpu.VMEM((3, wide, lat), f32),
            pltpu.VMEM((3, wide, lat), f32),
            pltpu.VMEM((3, wide, lat), f32),
            pltpu.VMEM((3, wide, lat), f32),
            pltpu.VMEM((2 * STEPS * cols, lat), f32),
            pltpu.VMEM((1, nobs), f32),
            pltpu.VMEM((max(ens - 1, 1), 1, nobs), f32),
            pltpu.VMEM((STEPS * cols, lat), f32),
            pltpu.VMEM((STEPS, wide, lat), f32),
            pltpu.VMEM((3, 8, lat), f32),
            pltpu.VMEM((max(ens - 1, 1), 3, 8, lat), f32),
            pltpu.VMEM((2, 8, lat), f32),
            pltpu.VMEM((2, 8, lat), f32),
            pltpu.VMEM((count - 1, 1, 128), f32),
            pltpu.VMEM((1, 128), f32),
            dma((10,)), dma((6,)), dma((4 + len(SHARES),)),
            dma, dma,
        ],
        compiler_params=pltpu.CompilerParams(
            collective_id=0, has_side_effects=True, vmem_limit_bytes=61 * 1024 * 1024
        ),
    )(
        control, direction, residual, ens_perturb, localize,
        obs_cell.reshape(1, nobs), obs_slot.reshape(1, nobs), obs_weight.reshape(1, nobs),
        jnp.asarray(grid_constants(lat)),
    )
    outs = pl.pallas_call(
        update,
        out_shape=[jax.ShapeDtypeStruct((members, cols, lat), f32)] * 3,
        in_specs=[vmem] * 5,
        out_specs=[hbm] * 3,
        scratch_shapes=[pltpu.VMEM((members, cols, lat), f32)] * 3 + [dma((3,))],
        compiler_params=pltpu.CompilerParams(vmem_limit_bytes=8 * 1024 * 1024),
    )(*outs)
    return tuple(map(flip, outs))


def solution(mesh):
    fields = P("ens", None, "lon")
    in_specs = (fields, fields, fields, P("ens", None, None, "lon"), P(), P("lon"), P("lon"), P("lon"))
    ens, lon = mesh.shape["ens"], mesh.shape["lon"]
    return jax.shard_map(
        functools.partial(body, ens, lon), mesh=mesh, in_specs=in_specs,
        out_specs=(fields, fields, fields), check_vma=False,
    )
```

```python
import functools
import itertools

import numpy as np
import jax
import jax.numpy as jnp
from jax import lax
from jax.experimental import pallas as pl
from jax.experimental.pallas import tpu as pltpu
from jax.sharding import PartitionSpec as P

STEPS = 3
HALO = 8
HALF = 0.5 * 0.35
SHARES = (0, 4, 8, 13, 16)
BLOCK = 256
MESH = pl.DeviceIdType.MESH
NT = (((1,), (1,)), ((), ()))
NN = (((1,), (0,)), ((), ()))


def split_bf16(values):
    high = values.astype(jnp.bfloat16)
    low = (values - high.astype(jnp.float32)).astype(jnp.bfloat16)
    return high, low


def dot(left, right, dims):
    return lax.dot_general(left, right, dims, preferred_element_type=jnp.float32)


def grid_constants(lat):
    phi = np.pi * (-1.0 / 3.0 + 2.0 / 3.0 * (np.arange(lat) + 0.5) / lat)
    rows = np.stack([HALF / np.cos(phi), 0.2 * np.sin(phi)])
    return np.ascontiguousarray(np.broadcast_to(rows[:, None], (2, 8, lat))).astype(np.float32)


def linear_step(source, target, sign, consts, blocks, low_end, high_end, rest=True, extra=None):
    panels = source.shape[2] // 128
    row = lax.broadcasted_iota(jnp.int32, (8, 128), 0)
    lane = lax.broadcasted_iota(jnp.int32, (8, 128), 1)

    def less(value, term):
        return value - term if sign > 0 else value + term

    for j in range(panels):
        lanes = pl.ds(128 * j, 128)
        lon_c, cor_c = consts[0, :, lanes], consts[1, :, lanes]

        def tile(comp, start, panel):
            return source[comp, pl.ds(start, 8), pl.ds(128 * panel, 128)]

        def lon_diff(comp, start, block):
            ahead = tile(comp, start + 8, j) if start + 8 < high_end else block
            behind = tile(comp, start - 8, j) if start > low_end else block
            east = pltpu.roll(jnp.where(row == 0, ahead, block), 7, 0)
            west = pltpu.roll(jnp.where(row == 7, behind, block), 1, 0)
            return lon_c * (east - west)

        def lat_diff(comp, start, block):
            ahead = tile(comp, start, j + 1) if j + 1 < panels else 0.0
            behind = tile(comp, start, j - 1) if j else 0.0
            up = pltpu.roll(jnp.where(lane == 0, ahead, block), 127, 1)
            down = pltpu.roll(jnp.where(lane == 127, behind, block), 1, 1)
            return HALF * (up - down)

        for start in blocks:
            here = pl.ds(start, 8)
            height = tile(0, start, j)
            along_lon, along_lat = lon_diff(0, start, height), lat_diff(0, start, height)
            if rest:
                zonal, merid = tile(1, start, j), tile(2, start, j)
                new = less(height, lon_diff(1, start, zonal) + lat_diff(2, start, merid))
                target[1, here, lanes] = less(zonal, along_lon - cor_c * merid)
                target[2, here, lanes] = less(merid, along_lat + cor_c * zonal)
            else:
                new = height
                target[1, here, lanes] = less(0.0, along_lon)
                target[2, here, lanes] = less(0.0, along_lat)
            target[0, here, lanes] = new if extra is None else new + extra[here, lanes]


def fold(values):
    values = values + pltpu.roll(values, 64, 1)
    return values + pltpu.roll(values, 32, 1)


def pack_rows(rows):
    lane = lax.broadcasted_iota(jnp.int32, (1, 128), 1) // 32
    packed = jnp.zeros((1, 128), jnp.float32)
    for k, row in enumerate(rows):
        packed = jnp.where(lane == k, fold(row), packed)
    return packed


def unpack_rows(total, number):
    lane = lax.broadcasted_iota(jnp.int32, (1, 128), 1) // 32
    return [
        jnp.sum(jnp.where(lane == k, total, 0.0), axis=1, keepdims=True) for k in range(number)
    ]


def lane_sum(values):
    total = values[:, :128]
    for k in range(128, values.shape[1], 128):
        total = total + values[:, k:k + 128]
    return total


LEFT_COPY, RIGHT_COPY, MASS_COPY, NEAR_COPY, LATE_COPY, SUM_COPY = range(6)


def side_rows():
    return [(n, k) for n in reversed(range(STEPS)) for k in range(n + 1)]


def kernel(
    ens, lon, control_hbm, direction_hbm, residual_hbm, perturb_hbm, localize_hbm, cell_hbm,
    slot_hbm, weight_hbm, consts_hbm,
    control, residual, direction, image, scalars,
    localize, perturb, cell, slot, weight, consts,
    high, low, split, onehot, state0, state1, state2, state3, heights, observed, arrived,
    spread, forcing, near, near_in, mass, mass_in, tiles, tile,
    load_sem, send_sem, recv_sem, tile_send, tile_recv,
):
    me_e, me_l = lax.axis_index("ens"), lax.axis_index("lon")
    members, cols, lat = direction.shape
    nobs = cell.shape[1]
    wide = state0.shape[1]
    stacked = members * cols
    slots_cols = STEPS * cols
    blocks = [pl.ds(k, BLOCK) for k in range(0, lat, BLOCK)]
    cuts = [nobs * share // SHARES[-1] for share in SHARES]
    chunks = [pl.ds(start, stop - start) for start, stop in zip(cuts, cuts[1:])]
    panels = range(lat // 128)

    def wrap(value, size):
        return jnp.where(value >= size, value - size, value)

    left_dev = (me_e, wrap(me_l + lon - 1, lon))
    right_dev = (me_e, wrap(me_l + 1, lon))

    load_ids = itertools.count()

    def load(src, dst):
        copy = pltpu.make_async_copy(src, dst, load_sem.at[next(load_ids)])
        copy.start()
        return copy

    load_obs = [load(cell_hbm, cell), load(slot_hbm, slot), load(weight_hbm, weight)]
    load_d = load(direction_hbm, direction)
    halves = [pl.ds(k, lat // 2) for k in (0, lat // 2)]
    load_l = [load(localize_hbm.at[halves[0]], localize.at[halves[0]])]
    load_p = load(perturb_hbm, perturb)
    load_l.append(load(localize_hbm.at[halves[1]], localize.at[halves[1]]))
    load_c = load(consts_hbm, consts)
    load_r = load(residual_hbm, residual)
    load_v = load(control_hbm, control)

    barrier = pltpu.get_barrier_semaphore()

    def remote(src, dst, device, kind, arrival):
        return pltpu.make_async_remote_copy(
            src_ref=src, dst_ref=dst, send_sem=send_sem.at[kind], recv_sem=recv_sem.at[arrival],
            device_id=device, device_id_type=MESH,
        )

    def all_of(ref, kind, arrival):
        return remote(ref, ref, right_dev, kind, arrival)

    order = sorted(range(lon), key=lambda l: (l == 0, min(l, lon - l), l))

    def each_peer(act):
        peers_e = [wrap(me_e + e, ens) for e in range(ens)]
        for l in order:
            peer_l = wrap(me_l + l, lon)
            for e in range(ens):
                if e or l:
                    act(e * lon + l - 1, (peers_e[e], peer_l))

    each_peer(lambda index, device: pl.semaphore_signal(
        barrier, inc=1, device_id=device, device_id_type=MESH
    ))

    for copy in load_obs:
        copy.wait()
    rows = (cell[...] // cols).reshape(nobs // 128, 128)
    rows = jnp.concatenate([rows] * (128 * 128 // nobs), axis=0).T
    lanes = lax.broadcasted_iota(jnp.int32, (16, 128), 1).astype(jnp.int16)
    one, zero = jnp.ones((16, 128), jnp.bfloat16), jnp.zeros((16, 128), jnp.bfloat16)

    def mark(groups):
        for group in groups:
            for s in range(0, 128, 16):
                row = jnp.broadcast_to(rows[s:s + 16, group:group + 1], (16, 128))
                row = row.astype(jnp.int16)
                for j in panels:
                    hit = row == lanes + jnp.int16(128 * j)
                    onehot[j, pl.ds(128 * group + s, 16), :] = jnp.where(hit, one, zero)

    groups = nobs // 128
    mark(range(0, groups // 2))

    def panel(ref, at, which=panels):
        return jnp.concatenate([ref[j, at, :] for j in which], axis=1)

    def store_panels(ref, at, values):
        for j in panels:
            ref[j, at, :] = values[:, 128 * j:128 * j + 128]

    load_d.wait()
    d_high, d_low = split_bf16(direction[...].reshape(stacked, lat))

    edge = 2 * STEPS
    own = pl.ds(HALO, cols)
    first, last = pl.ds(HALO, edge), pl.ds(HALO + cols - edge, edge)
    before, after = pl.ds(HALO - edge, edge), pl.ds(HALO + cols, edge)
    d_both = jnp.concatenate([d_high, d_low], axis=0)
    mark(range(groups // 2, groups * 3 // 4))
    for k, at in enumerate(blocks):
        if k % (len(blocks) // 2) == 0:
            load_l[k // (len(blocks) // 2)].wait()
            if k == 0:
                load_p.wait()
        l_high, l_low = split_bf16(localize[at, :])
        store_panels(high, at, l_high)
        store_panels(low, at, l_low)
        both = dot(d_both, l_high, NT)
        local = both[:stacked] + both[stacked:] + dot(d_high, l_low, NT)
        for c in range(3):
            total = None
            for m in range(members):
                term = perturb[m, c, :, at].astype(jnp.float32) * local[m * cols:(m + 1) * cols]
                total = term if total is None else total + term
            state0[c, own, at] = total
        mark(range(groups * (12 + k) // 16, groups * (13 + k) // 16))
    def keys(at):
        cells, slots = cell[:, at], slot[:, at]
        return slots * cols + (cells - cells // cols * cols)

    def scattered(hit, values):
        v_high = values.astype(jnp.bfloat16).astype(jnp.float32)
        return jnp.concatenate(
            [jnp.where(hit, v_high, 0.0), jnp.where(hit, values - v_high, 0.0)], axis=0
        ).astype(jnp.bfloat16)

    load_c.wait()
    load_r.wait()
    states = (state0, state1, state2, state3)

    def keep(n, starts):
        for start in starts:
            value = states[n + 1][0, pl.ds(start, 8), :]
            v_high = value.astype(jnp.bfloat16).astype(jnp.float32)
            row = n * cols + start - HALO
            heights[pl.ds(row, 8), :] = v_high
            heights[pl.ds(slots_cols + row, 8), :] = value - v_high

    inner = range(HALO, HALO + cols, 8)
    def side_ids(width):
        row = lax.broadcasted_iota(jnp.int32, (16, 128), 0)
        result = jnp.full((16, 128), -1, jnp.int32)
        for k, (n, dist) in enumerate(side_rows()):
            result = jnp.where(row == k, n * cols + dist, result)
            result = jnp.where(row == 8 + k, n * cols + cols - 1 - n + dist, result)
        return jnp.concatenate([result] * (width // 128), axis=1)


    def before_halo():
        for n in range(STEPS):
            linear_step(states[n], states[n + 1], 1, consts, inner, HALO, HALO + cols)
            keep(n, inner)

        left = scattered(side_ids(nobs) == keys(pl.ds(0, nobs)), weight[...])
        both = dot(left, panel(onehot, pl.ds(0, nobs)), NN)
        mass[...] = (both[:16] + both[16:]).reshape(2, 8, lat)

    is_first = (me_l == 0) & (me_e == 0)
    pl.when(is_first)(before_halo)

    pl.semaphore_wait(barrier, ens * lon - 1)
    f_copies = [
        remote(state0.at[:, first], state0.at[:, after], left_dev, LEFT_COPY, 0),
        remote(state0.at[:, last], state0.at[:, before], right_dev, RIGHT_COPY, 1),
    ]
    for copy in f_copies:
        copy.start()

    pl.when(jnp.logical_not(is_first))(before_halo)
    norm_old = jnp.zeros((8, 128), jnp.float32)
    for at in blocks:
        value = residual[:, :, at]
        norm_old += lane_sum((value * value).reshape(stacked // 8, 8, BLOCK).sum(axis=0))

    used = pl.ds(0, len(side_rows()))
    m_copies = [
        remote(mass.at[0, used], mass_in.at[1, used], left_dev, MASS_COPY, 2),
        remote(mass.at[1, used], mass_in.at[0, used], right_dev, MASS_COPY, 2),
    ]
    for copy in m_copies:
        copy.start()

    is_left, is_right = me_l == 0, me_l == lon - 1
    is_end = is_left | is_right
    key_ids = lax.broadcasted_iota(jnp.int32, (slots_cols, nobs), 0)
    tall = 2 if ens % 2 == 0 else 1
    broad = ens // tall
    me_a = me_e // broad
    me_b = me_e - me_a * broad
    straight = [(0, j) for j in range(1, broad)] + [(i, 0) for i in range(1, tall)]
    slanted = [(i, j) for i in range(1, tall) for j in range(1, broad)]
    peers = [
        (wrap(me_a + i, tall) * broad + wrap(me_b + j, broad), me_l)
        for i, j in straight + slanted
    ]
    n_copies = [
        [
            remote(near.at[part, used], near_in.at[j, part, used], peer, kind, arrival)
            for part, kind, arrival in ((0, NEAR_COPY, 3), (1, NEAR_COPY, 3), (2, LATE_COPY, 4))
        ]
        for j, peer in enumerate(peers)
    ]
    sums = {
        (j, k): remote(observed.at[:, at], arrived.at[j, :, at], peer, SUM_COPY, 5 + k)
        for k, at in enumerate(chunks) for j, peer in enumerate(peers)
    }
    far = (is_left, is_right)
    own_edge = (
        lambda n, dist: HALO + dist,
        lambda n, dist: HALO + cols - 1 - n + dist,
    )
    beyond = (
        lambda n, dist: HALO - 1 - n + dist,
        lambda n, dist: HALO + cols + dist,
    )

    def outer(side):
        starts = (HALO + cols - 8, HALO + cols) if side else (0, HALO)
        f_copies[1 - side].wait_recv()
        for n in range(STEPS):
            linear_step(states[n], states[n + 1], 1, consts, starts, 0, wide)
            keep(n, starts[:1] if side else starts[1:])
        for k, (n, dist) in enumerate(side_rows()):
            near[side, pl.ds(k, 1), :] = states[n + 1][0, pl.ds(beyond[side](n, dist), 1), :]

    def outer_late(side):
        outer(side)
        for k, (n, dist) in enumerate(side_rows()):
            near[2, pl.ds(k, 1), :] = states[n + 1][0, pl.ds(own_edge[side](n, dist), 1), :]
        for parts in n_copies:
            parts[side].start()
            parts[2].start()

    for side in range(2):
        @pl.when(jnp.logical_not(far[side]))
        def _():
            outer(side)
            for parts in n_copies[:len(straight)]:
                parts[side].start()

    first_own = jnp.where(is_left, 0, -cols)
    last_own = jnp.where(is_right, cols - 1, 2 * cols)

    def gather(which, after_first):
        table = heights[...].astype(jnp.bfloat16)

        def finish(k, both):
            at = chunks[k]
            slots, key = slot[:, at], keys(at)
            col = key - slots * cols
            late = (col <= slots + first_own) | (col >= last_own - slots)
            both = both[:slots_cols] + both[slots_cols:]
            hit = key_ids[:, :both.shape[1]] == jnp.where(late, -1, key)
            observed[:, at] = jnp.sum(jnp.where(hit, both, 0.0), axis=0, keepdims=True)
            for j in range(ens - 1):
                sums[j, k].start()
            if k == 0:
                after_first()

        ahead = None
        for k in which:
            both = dot(table, panel(onehot, chunks[k]), NT)
            if ahead is not None:
                finish(*ahead)
            ahead = (k, both)
        finish(*ahead)

    number = len(chunks)

    def slanted_start(sides):
        for parts in n_copies[len(straight):]:
            for side in sides:
                parts[side].start()

    @pl.when(is_end)
    def _():
        gather(range(number - 1), lambda: None)
        for side in range(2):
            @pl.when(far[side])
            def _():
                slanted_start((1 - side,))
                outer_late(side)
        gather(range(number - 1, number), lambda: None)

    @pl.when(jnp.logical_not(is_end))
    def _():
        gather(range(number), lambda: slanted_start(range(2)))

    for k, at in enumerate(chunks):
        all_of(arrived.at[:, :, at], SUM_COPY, 5 + k).wait_recv()
        total = observed[:, at]
        for j in range(ens - 1):
            total = total + arrived[j, :, at]
        left = scattered(key_ids[:, :total.shape[1]] == keys(at), weight[:, at] * total)
        both = dot(left, panel(onehot, at), NN)
        both = both[:slots_cols] + both[slots_cols:]
        if k == 0:
            spread[...] = both
        elif k < len(chunks) - 1:
            spread[...] += both
        else:
            both = spread[...] + both
            for s in range(STEPS):
                forcing[s, own, :] = both[s * cols:(s + 1) * cols]

    both_sides = pl.ds(0, 2)
    m_all = all_of(mass_in.at[:, used], MASS_COPY, 2)
    n_all = all_of(near_in.at[:, both_sides, used], NEAR_COPY, 3)
    late_all = all_of(near_in.at[:, 2, used], LATE_COPY, 4)
    m_all.wait_recv()
    n_all.wait_recv()

    def summed(part):
        total = near[part]
        for j in range(ens - 1):
            total = total + near_in[j, part]
        return total

    for side in range(2):
        made = summed(side) * mass_in[side]
        for k, (n, dist) in enumerate(side_rows()):
            forcing[n, pl.ds(beyond[side](n, dist), 1), :] = made[k:k + 1]

        @pl.when(far[side])
        def _():
            late_all.wait_recv()
            made = summed(2) * mass[side]
            for k, (n, dist) in enumerate(side_rows()):
                forcing[n, pl.ds(own_edge[side](n, dist), 1), :] = made[k:k + 1]
    every = range(0, wide, 8)
    linear_step(forcing.at[pl.ds(2, 1)], state1, -1, consts, every, 0, wide, False, forcing.at[1])
    linear_step(state1, state2, -1, consts, every, 0, wide, True, forcing.at[0])
    linear_step(state2, state3, -1, consts, inner, 0, wide)

    for m in range(members):
        total = None
        for c in range(3):
            term = perturb[m, c].astype(jnp.float32) * state3[c, own, :]
            total = term if total is None else total + term
        p_high, p_low = split_bf16(total)
        store_panels(split, pl.ds(m * cols, cols), p_high)
        store_panels(split, pl.ds(stacked + m * cols, cols), p_low)

    p_both = panel(split, pl.ds(0, 2 * stacked))
    sums_new = [norm_old] + [jnp.zeros((8, 128), jnp.float32)] * 3
    for k, at in enumerate(blocks):
        pair = range(k * BLOCK // 128, (k + 1) * BLOCK // 128)
        both = dot(p_both, panel(high, pl.ds(0, lat), pair), NN)
        back = both[:stacked] + both[stacked:]
        back += dot(p_both[:stacked], panel(low, pl.ds(0, lat), pair), NN)
        d = direction[:, :, at].reshape(stacked, BLOCK)
        r = residual[:, :, at].reshape(stacked, BLOCK)
        img = d + back
        image[:, :, at] = img.reshape(members, cols, BLOCK)
        for j, term in enumerate((d * img, r * img, img * img)):
            sums_new[j + 1] += lane_sum(term.reshape(stacked // 8, 8, BLOCK).sum(axis=0))

    tile[...] = pack_rows([jnp.sum(value, axis=0, keepdims=True) for value in sums_new])

    def tell(index, device):
        pltpu.make_async_remote_copy(
            src_ref=tile, dst_ref=tiles.at[index], send_sem=tile_send, recv_sem=tile_recv,
            device_id=device, device_id_type=MESH,
        ).start()

    each_peer(tell)
    load_v.wait()
    for copy in f_copies:
        copy.wait_send()
    all_of(arrived, SUM_COPY, 5).wait_send()
    m_all.wait_send()
    n_all.wait_send()
    pl.when(is_end)(late_all.wait_send)
    everything = pltpu.make_async_remote_copy(
        src_ref=tiles, dst_ref=tiles, send_sem=tile_send, recv_sem=tile_recv,
        device_id=right_dev, device_id_type=MESH,
    )
    everything.wait_send()
    everything.wait_recv()
    norm_old, curvature, cross_term, square = unpack_rows(
        jnp.sum(tiles[...], axis=0) + tile[...], 4
    )
    step_size = norm_old / curvature
    norm_new = norm_old - 2.0 * step_size * cross_term + step_size * step_size * square
    scalars[pl.ds(0, 1), :] = jnp.broadcast_to(step_size, (1, 128))
    scalars[pl.ds(1, 1), :] = jnp.broadcast_to(norm_new / norm_old, (1, 128))


def update(
    control, residual, direction, image, scalars, control_out, residual_out, direction_out,
    control_new, residual_new, direction_new, sem,
):
    step_size, ratio = scalars[pl.ds(0, 1), pl.ds(0, 1)], scalars[pl.ds(1, 1), pl.ds(0, 1)]

    def copy(which, src, dst, *at):
        part = (src.at[at], dst.at[at]) if at else (src, dst)
        return pltpu.make_async_copy(*part, sem.at[which])

    pairs = (
        (residual_new, residual_out), (direction_new, direction_out), (control_new, control_out)
    )
    members, cols = control.shape[:2]
    for m in range(members):
        for h in range(2):
            at = (m, pl.ds(h * cols // 2, cols // 2))
            d = direction[at]
            new = residual[at] - step_size * image[at]
            residual_new[at] = new
            direction_new[at] = new + ratio * d
            control_new[at] = control[at] + step_size * d
            for which, pair in enumerate(pairs):
                copy(which, *pair, *at).start()
    for which, pair in enumerate(pairs):
        copy(which, *pair).wait()


def body(ens, lon, control, residual, direction, ens_perturb, localize, obs_cell, obs_slot, obs_weight):
    flip = functools.partial(jnp.swapaxes, axis1=-1, axis2=-2)
    control, residual, direction, ens_perturb = map(flip, (control, residual, direction, ens_perturb))
    members, cols, lat = direction.shape
    nobs = obs_cell.shape[0]
    count = ens * lon
    wide = cols + 2 * HALO
    f32, bf16, i32 = jnp.float32, jnp.bfloat16, jnp.int32
    hbm = pl.BlockSpec(memory_space=pltpu.HBM)
    dma = pltpu.SemaphoreType.DMA
    field = pltpu.VMEM((members, cols, lat), f32)
    vmem = pl.BlockSpec(memory_space=pltpu.VMEM)
    outs = pl.pallas_call(
        functools.partial(kernel, ens, lon),
        out_shape=(field, field, field, field, pltpu.VMEM((8, 128), f32)),
        in_specs=[hbm] * 9,
        out_specs=(vmem,) * 5,
        scratch_shapes=[
            pltpu.VMEM((lat, lat), f32),
            pltpu.VMEM((members, 3, cols, lat), bf16),
            pltpu.VMEM((1, nobs), i32),
            pltpu.VMEM((1, nobs), i32),
            pltpu.VMEM((1, nobs), f32),
            pltpu.VMEM((2, 8, lat), f32),
            pltpu.VMEM((lat // 128, lat, 128), bf16),
            pltpu.VMEM((lat // 128, lat, 128), bf16),
            pltpu.VMEM((lat // 128, 2 * members * cols, 128), bf16),
            pltpu.VMEM((lat // 128, nobs, 128), bf16),
            pltpu.VMEM((3, wide, lat), f32),
            pltpu.VMEM((3, wide, lat), f32),
            pltpu.VMEM((3, wide, lat), f32),
            pltpu.VMEM((3, wide, lat), f32),
            pltpu.VMEM((2 * STEPS * cols, lat), f32),
            pltpu.VMEM((1, nobs), f32),
            pltpu.VMEM((max(ens - 1, 1), 1, nobs), f32),
            pltpu.VMEM((STEPS * cols, lat), f32),
            pltpu.VMEM((STEPS, wide, lat), f32),
            pltpu.VMEM((3, 8, lat), f32),
            pltpu.VMEM((max(ens - 1, 1), 3, 8, lat), f32),
            pltpu.VMEM((2, 8, lat), f32),
            pltpu.VMEM((2, 8, lat), f32),
            pltpu.VMEM((count - 1, 1, 128), f32),
            pltpu.VMEM((1, 128), f32),
            dma((10,)), dma((6,)), dma((4 + len(SHARES),)),
            dma, dma,
        ],
        compiler_params=pltpu.CompilerParams(
            collective_id=0, has_side_effects=True, vmem_limit_bytes=61 * 1024 * 1024
        ),
    )(
        control, direction, residual, ens_perturb, localize,
        obs_cell.reshape(1, nobs), obs_slot.reshape(1, nobs), obs_weight.reshape(1, nobs),
        jnp.asarray(grid_constants(lat)),
    )
    outs = pl.pallas_call(
        update,
        out_shape=[jax.ShapeDtypeStruct((members, cols, lat), f32)] * 3,
        in_specs=[vmem] * 5,
        out_specs=[hbm] * 3,
        scratch_shapes=[pltpu.VMEM((members, cols, lat), f32)] * 3 + [dma((3,))],
        compiler_params=pltpu.CompilerParams(vmem_limit_bytes=8 * 1024 * 1024),
    )(*outs)
    return tuple(map(flip, outs))


def solution(mesh):
    fields = P("ens", None, "lon")
    in_specs = (fields, fields, fields, P("ens", None, None, "lon"), P(), P("lon"), P("lon"), P("lon"))
    ens, lon = mesh.shape["ens"], mesh.shape["lon"]
    return jax.shard_map(
        functools.partial(body, ens, lon), mesh=mesh, in_specs=in_specs,
        out_specs=(fields, fields, fields), check_vma=False,
    )
```
